32 devices in a mesh: groups: 2 (over y), shell: 8 (over z, x), batch: 2 (over core).
Axes of the slice: x: 2, y: 2, z: 4, core: 2. Of those that a mesh axis runs over, the one named last changes fastest.
Arguments:
- particles: bfloat16 [320, 1024], P(('groups', 'batch'), 'shell'), parts along dimension 0, may hold values from -5 to 5
- classes: bfloat16 [512, 1024], P('groups', 'shell'), parts along dimension 0, may hold values from -2.5 to 2.5
- ctf: float32 [16, 512], P('groups', 'shell'), parts along dimension 0, may hold values from 0.1 to 1
- sigma2: float32 [128], P('groups'), parts along dimension 0, may hold values from 0.5 to 8
- shell_of: int32 [512], P('shell'), may hold values from 0 to 63, as said below
- rot_table: int32 [48, 512], P(None, 'shell'), may hold values from 0 to 511, as said below
- ctf_group: int32 [320], P(('groups', 'batch')), parts along dimension 0, may hold values from 0 to 7
Outputs:
- class_sums: float32 [512, 1024], P('groups', 'shell'), parts along dimension 0
- class_weights: float32 [512, 512], P('groups', 'shell'), parts along dimension 0
- log_evidence: float32 [320], P(('groups', 'batch')), parts along dimension 0
The draws below stay inside these ranges and needn't reach their ends.
There are 2 independent parts, one for each index of `groups`. The reference program is written for one: setup_inputs(seed, part) draws one part's arguments, and reference() takes and returns one part's arrays. A program takes and returns all parts, laid end to end along the dimension named above; an argument that names none is the same for every part. Nothing has to cross between parts.
Inputs may be any that keep to these rules, and one draw needn't show every extreme that they name: shell_of never falls along the coefficients; its first entry is 0 and its last 63. `rot_table`: for each rotation, each aligned block of 64 coefficients is mapped onto itself one to one; rotation 0 maps every coefficient to itself.
All inputs are finite; a program needn't handle non-finite values.
Results may differ from the reference program's by a relative error of at most 0.0041.
Values may be sent and summed in bfloat16 or wider, within the bound.
A program may use at most 64 MiB of HBM per device.

```python
import math
import jax
import jax.numpy as jnp
from jax import lax

K = 256
ROT = 48
CO_DEV = 64
SHELLS = 64
CTFG = 8
COEF = 512
PARTICLES = 160
N_SHELL = 8


def particle_field(key):
    shape = (PARTICLES, 2 * COEF)
    return jnp.clip(jax.random.normal(jax.random.fold_in(key, 11), shape, jnp.float32), -5.0, 5.0)


def draw_particles(key, part):
    return particle_field(key).astype(jnp.bfloat16)


def draw_classes(key, part):
    noise = jnp.clip(jax.random.normal(jax.random.fold_in(key, 21), (K, 2 * COEF), jnp.float32), -5.0, 5.0) * 0.02
    return noise.astype(jnp.bfloat16)


def draw_shell_of(key, part):
    values = jnp.sort(jax.random.randint(key, (COEF,), 0, SHELLS, dtype=jnp.int32))
    values = values.at[0].set(0).at[COEF - 1].set(SHELLS - 1)
    return values.astype(jnp.int32)


def draw_rot_table(key, part):
    blocks = COEF // CO_DEV
    ranks = jnp.arange(CO_DEV, dtype=jnp.int32)
    keyed = jax.random.randint(key, (ROT, blocks, CO_DEV), 0, 1048576, dtype=jnp.int32) * CO_DEV + ranks
    order = jnp.argsort(keyed, axis=-1, stable=True).astype(jnp.int32)
    identity = jnp.broadcast_to(ranks, (blocks, CO_DEV))
    order = order.at[0].set(identity)
    offsets = (jnp.arange(blocks, dtype=jnp.int32) * CO_DEV)[None, :, None]
    return (order + offsets).reshape(ROT, COEF).astype(jnp.int32)


def touch_ends(values, stream_key, least, high):
    longest = values.shape.index(max(values.shape))
    spots = []
    for shift in (0, 1):
        where = [jax.random.randint(jax.random.fold_in(stream_key, axis), (), 0, length) for axis, length in enumerate(values.shape)]
        where[longest] = (where[longest] + shift) % values.shape[longest]
        spots.append(tuple(where))
    return values.at[spots[0]].set(least).at[spots[1]].set(high)


def levels(own_key, extent, split, low, high):
    factor_of, own = 1.0, jax.random.fold_in(own_key, 6)
    for dim, shards_of in split:
        draws = jnp.exp(jax.random.uniform(jax.random.fold_in(own, dim), (shards_of,), jnp.float32, low / len(split), high / len(split)))
        factor_of = factor_of * jnp.repeat(draws, extent[dim] // shards_of).reshape([-1 if axis == dim else 1 for axis in range(len(extent))])
    return factor_of


def setup_inputs(seed: int = 0, part: int = 0) -> dict:
    seeds = jax.random.split(jax.random.key(seed), 8)
    own_keys = jax.random.split(jax.random.fold_in(seeds[7], part), 8)
    return {
        "particles": draw_particles(jax.random.fold_in(jax.random.fold_in(seeds[7], part), 71), part),
        "classes": draw_classes(jax.random.fold_in(jax.random.fold_in(seeds[7], part), 71), part),
        "ctf": jnp.clip(0.1 + 0.9 * jax.random.uniform(own_keys[2], (CTFG, COEF), jnp.float32) ** levels(own_keys[2], (CTFG, COEF), ((1, 8),), -0.2, 0.2), 0.1, 1.0),
        "sigma2": jnp.clip(jnp.exp(jax.random.uniform(own_keys[3], (SHELLS,), jnp.float32, math.log(0.5), math.log(8.0))), 0.5, 8.0),
        "shell_of": draw_shell_of(jax.random.fold_in(seeds[7], 71), part),
        "rot_table": draw_rot_table(jax.random.fold_in(seeds[7], 71), part),
        "ctf_group": touch_ends(jax.random.randint(own_keys[6], (PARTICLES,), 0, CTFG), jax.random.fold_in(own_keys[6], 1), 0, CTFG - 1).astype(jnp.int32),
    }


def halves(array):
    rows = array.shape[0]
    blocks = array.reshape(rows, N_SHELL, 2, CO_DEV)
    return blocks[:, :, 0, :].reshape(rows, COEF), blocks[:, :, 1, :].reshape(rows, COEF)


def join_parts(real_part, imag_part):
    rows = real_part.shape[0]
    stacked = jnp.stack([real_part.reshape(rows, N_SHELL, CO_DEV), imag_part.reshape(rows, N_SHELL, CO_DEV)], axis=2)
    return stacked.reshape(rows, 2 * COEF)


def reference(particles, classes, ctf, sigma2, shell_of, rot_table, ctf_group):
    highest = lax.Precision.HIGHEST
    weight = 1.0 / sigma2[shell_of]
    real_part, imag_part = halves(particles.astype(jnp.float32))
    class_real, class_imag = halves(classes)
    ctf_part = ctf[ctf_group]
    weighted_ctf = weight[None, :] * ctf_part
    weighted_real = (weighted_ctf * real_part).astype(jnp.bfloat16)
    weighted_imag = (weighted_ctf * imag_part).astype(jnp.bfloat16)
    ctf_power = weight[None, :] * ctf * ctf

    def score_rotation(table_row):
        rot_real = class_real[:, table_row]
        rot_imag = class_imag[:, table_row]
        cross_terms = jnp.dot(weighted_real, rot_real.T, preferred_element_type=jnp.float32)
        cross_terms = cross_terms + jnp.dot(weighted_imag, rot_imag.T, preferred_element_type=jnp.float32)
        class_power = rot_real.astype(jnp.float32) ** 2 + rot_imag.astype(jnp.float32) ** 2
        penalty = jnp.dot(ctf_power, class_power.T, precision=highest, preferred_element_type=jnp.float32)
        return cross_terms - 0.5 * penalty[ctf_group]

    scores = lax.map(score_rotation, rot_table)
    scores = jnp.transpose(scores, (1, 2, 0)).reshape(PARTICLES, K * ROT)
    peak = jnp.max(scores, axis=1)
    log_evidence = peak + jnp.log(jnp.sum(jnp.exp(scores - peak[:, None]), axis=1))
    posterior = jnp.exp(scores - log_evidence[:, None]).astype(jnp.bfloat16).reshape(PARTICLES, K, ROT)
    sources = jnp.concatenate([ctf_part * real_part, ctf_part * imag_part, ctf_part * ctf_part], axis=1).astype(jnp.bfloat16)

    def add_rotation(totals, inputs):
        post_rot, table_row = inputs
        frame = jnp.dot(post_rot.T, sources, preferred_element_type=jnp.float32).reshape(K, 3, COEF)
        return totals.at[:, :, table_row].add(frame), None

    totals, unused = lax.scan(add_rotation, jnp.zeros((K, 3, COEF), jnp.float32), (jnp.transpose(posterior, (2, 0, 1)), rot_table))
    class_sums = join_parts(totals[:, 0], totals[:, 1])
    return class_sums, totals[:, 2], log_evidence
```

```python
import functools

import jax
import jax.numpy as jnp
from jax import lax
from jax.experimental import pallas as pl
from jax.experimental.pallas import tpu as pltpu
from jax.sharding import PartitionSpec as P

MESH = pl.DeviceIdType.MESH
BF16 = jnp.bfloat16
F32 = jnp.float32


def plain_body(particles, classes, ctf, sigma2, shell_of, rot_table, ctf_group):
    highest = lax.Precision.HIGHEST
    coef_width = shell_of.shape[0]
    class_count = classes.shape[0]
    rotations = rot_table.shape[0]
    levels = sigma2.shape[0]
    group_count = ctf.shape[0]
    offset = lax.axis_index("shell") * coef_width
    local_table = rot_table - offset
    pick_shell = (shell_of[:, None] == jnp.arange(levels, dtype=jnp.int32)[None, :]).astype(F32)
    weight = 1.0 / jnp.dot(pick_shell, sigma2, precision=highest, preferred_element_type=F32)
    pick_group = (ctf_group[:, None] == jnp.arange(group_count, dtype=jnp.int32)[None, :]).astype(F32)
    ctf_part = jnp.dot(pick_group, ctf, precision=highest, preferred_element_type=F32)
    values = particles.astype(F32)
    real_part = values[:, :coef_width]
    imag_part = values[:, coef_width:]
    weighted_ctf = weight[None, :] * ctf_part
    weighted = jnp.concatenate([weighted_ctf * real_part, weighted_ctf * imag_part], axis=1).astype(BF16)
    ctf_power = weight[None, :] * ctf * ctf
    sources = jnp.concatenate(
        [ctf_part * real_part, ctf_part * imag_part, ctf_part * ctf_part], axis=1
    ).astype(BF16)
    class_view = classes.reshape(class_count, 2, coef_width)
    rotated = jnp.take(class_view, local_table, axis=2)
    rotated = jnp.transpose(rotated, (0, 2, 1, 3)).reshape(class_count * rotations, 2 * coef_width)
    cross_terms = lax.dot_general(
        weighted, rotated, (((1,), (1,)), ((), ())), preferred_element_type=F32
    )
    rot_float = rotated.astype(F32)
    class_power = rot_float[:, :coef_width] ** 2 + rot_float[:, coef_width:] ** 2
    penalty = lax.dot_general(
        ctf_power, class_power, (((1,), (1,)), ((), ())), precision=highest, preferred_element_type=F32
    )
    total = lax.psum(
        cross_terms - 0.5 * jnp.dot(pick_group, penalty, precision=highest, preferred_element_type=F32),
        "shell",
    )
    peak = jnp.max(total, axis=1)
    log_evidence = peak + jnp.log(jnp.sum(jnp.exp(total - peak[:, None]), axis=1))
    posterior = jnp.exp(total - log_evidence[:, None]).astype(BF16)
    frames = lax.dot_general(
        posterior, sources, (((0,), (0,)), ((), ())), preferred_element_type=F32
    )
    frames = frames.reshape(class_count, rotations, 3, coef_width)
    placing = (
        local_table[:, :, None] == jnp.arange(coef_width, dtype=jnp.int32)[None, None, :]
    ).astype(F32)
    unrotated = jnp.einsum(
        "krqc,rcd->kqd", frames, placing, precision=highest, preferred_element_type=F32
    )
    sums_part = unrotated[:, 0:2].reshape(class_count, 2 * coef_width)
    weights_part = unrotated[:, 2]
    class_sums, class_weights = lax.psum((sums_part, weights_part), "batch")
    return (class_sums, class_weights, log_evidence)


def split3(x):
    one = x.astype(BF16).astype(F32)
    two = (x - one).astype(BF16).astype(F32)
    return one, two, x - one - two


def gather_lanes(x, index):
    return jnp.take_along_axis(x, index, axis=1, mode="promise_in_bounds")


def kernel(
    n, m, kc, rot, part_ref, tab_ref, cls_ref, cw_ref, pick_ref,
    sums_ref, wts_ref, logev_ref,
    g_part, g_tab, g_cls, g_cw, g_pick, fwd, inv, cls32, w_s, s_s, p_s, r_s, hi_s, lo_s, sc_s, post_s, frame,
    st_mine, st_all, o_mine, o_all,
    in_send, in_recv, relay_send, relay_recv, pick_sem, st_send, st_recv, o_send, o_recv,
):
    s = lax.axis_index("shell")
    b = lax.axis_index("batch")
    rows = part_ref.shape[0]
    total_rows = m * rows
    half = 64
    me = s * m + b
    nd = n * m
    lane = lambda shape: lax.broadcasted_iota(jnp.int32, shape, len(shape) - 1)

    def peer(o):
        other = lax.rem(me + o, nd)
        return other, {"shell": other // m, "batch": lax.rem(other, m)}

    barrier = pltpu.get_barrier_semaphore()
    for o in range(1, nd):
        pl.semaphore_signal(barrier, inc=1, device_id=peer(o)[1], device_id_type=MESH)
    pl.semaphore_wait(barrier, nd - 1)

    copies = []
    for o in range(1, n):
        t = lax.rem(s + o, n)
        dest = {"shell": t, "batch": b}
        first = pl.multiple_of((t * m + b) * kc, kc)
        pairs = (
            (cls_ref.at[pl.ds(first, kc)], g_cls.at[s]),
            (cw_ref, g_cw.at[s]),
            (tab_ref, g_tab.at[s]),
            (part_ref, g_part.at[b, s]),
        )
        for j, (src, dst) in enumerate(pairs):
            copy = pltpu.make_async_remote_copy(
                src_ref=src, dst_ref=dst, send_sem=in_send.at[j, t], recv_sem=in_recv.at[j, s],
                device_id=dest, device_id_type=MESH,
            )
            copy.start()
            copies.append(copy)
    partner = {"shell": s, "batch": 1 - b}
    pick_copy = pltpu.make_async_remote_copy(
        src_ref=pick_ref, dst_ref=g_pick.at[b], send_sem=pick_sem.at[0], recv_sem=pick_sem.at[1],
        device_id=partner, device_id_type=MESH,
    )
    pick_copy.start()
    relays = []

    def relay(src, t):
        copy = pltpu.make_async_remote_copy(
            src_ref=src, dst_ref=g_part.at[b, t], send_sem=relay_send.at[t], recv_sem=relay_recv.at[t],
            device_id=partner, device_id_type=MESH,
        )
        copy.start()
        relays.append(copy)

    relay(part_ref, s)
    g_part[b, s] = part_ref[...]
    g_pick[b] = pick_ref[...]
    g_tab[s] = tab_ref[...]
    g_cw[s] = cw_ref[...]
    g_cls[s] = cls_ref[pl.ds(pl.multiple_of(me * kc, kc), kc), :]

    def arrive(j, t):
        refs = (g_cls.at[t], g_cw.at[t], g_tab.at[t], g_part.at[b, t])
        pltpu.make_async_remote_copy(
            src_ref=refs[j], dst_ref=refs[j], send_sem=in_send.at[j, t], recv_sem=in_recv.at[j, t],
            device_id=partner, device_id_type=MESH,
        ).wait_recv()

    for o in range(1, n):
        t = lax.rem(s + n - o, n)
        arrive(0, t)
        arrive(1, t)
        arrive(2, t)
    for o in range(1, n):
        t = lax.rem(s + n - o, n)
        arrive(3, t)
        relay(g_part.at[b, t], t)

    left = lane((rot, 128)) < half
    for t in range(n):
        tab = g_tab[t].astype(F32)
        swap = pltpu.roll(tab, half, 1)
        fwd[t] = jnp.where(left, tab, swap + half).astype(jnp.int32)
        inv[t] = jnp.where(left, swap, tab + half).astype(jnp.int32)
        cls32[t] = g_cls[t].astype(F32)

    def rotate(r, carry):
        at = pl.ds(pl.multiple_of(r * kc, kc), kc)
        for t in range(n):
            index = jnp.broadcast_to(fwd[t, pl.ds(r, 1), :], (kc, 128))
            turned = gather_lanes(cls32[t], index)
            square = turned * turned
            high = square.astype(BF16)
            cols = slice(t * 128, t * 128 + 128)
            r_s[at, cols] = turned.astype(BF16)
            hi_s[at, cols] = high
            lo_s[at, cols] = (square - high.astype(F32)).astype(BF16)
        return carry

    lax.fori_loop(0, rot, rotate, 0)

    pick_copy.wait()
    for o in range(n):
        t = lax.rem(s + o, n)
        pltpu.make_async_remote_copy(
            src_ref=g_part.at[1 - b, t], dst_ref=g_part.at[1 - b, t],
            send_sem=relay_send.at[t], recv_sem=relay_recv.at[t],
            device_id=partner, device_id_type=MESH,
        ).wait_recv()

    pick = g_pick[...].reshape(total_rows, 128)[:, :32]
    left8 = lane((8, 128)) < half
    left_p = lane((total_rows, 128)) < half
    before = None
    for t in range(n):
        packed = g_cw[t]
        swap = pltpu.roll(packed, half, 1)
        ctf = jnp.where(left8, packed, swap)
        weight = jnp.where(left8, swap, packed)
        zero = jnp.zeros_like(ctf)
        pieces = jnp.concatenate(split3(ctf) + (zero,), axis=0).astype(BF16)
        ctf_part = jnp.dot(pick, pieces, preferred_element_type=F32)
        values = g_part[:, t].reshape(total_rows, 128).astype(F32)
        cols = slice(t * 128, t * 128 + 128)
        w_s[:, cols] = (weight[0:1] * ctf_part * values).astype(BF16)
        s_s[:, cols] = (ctf_part * values).astype(BF16)
        p_s[:, cols] = jnp.concatenate(split3(weight * ctf * ctf) + (zero,), axis=0).astype(BF16)
        if t % 2 == 1:
            mixed = jnp.where(left_p, before, ctf_part)
            cols = slice(n * 128 + t // 2 * 128, n * 128 + t // 2 * 128 + 128)
            s_s[:, cols] = (mixed * mixed).astype(BF16)
        before = ctf_part

    nt = (((1,), (1,)), ((), ()))
    chunk = 128
    big = kc * rot

    def score(i, peak):
        at = pl.ds(pl.multiple_of(i * chunk, chunk), chunk)
        cross = lax.dot_general(r_s[at, :], w_s[...], nt, preferred_element_type=F32)
        pen = lax.dot_general(hi_s[at, :], p_s[...], nt, preferred_element_type=F32)
        pen = pen + lax.dot_general(lo_s[at, :], p_s[...], nt, preferred_element_type=F32)
        spread = 0.0
        for piece in split3(pen):
            spread = spread + lax.dot_general(piece.astype(BF16), pick, nt, preferred_element_type=F32)
        total = cross - 0.5 * spread
        sc_s[at, :] = total
        return jnp.maximum(peak, jnp.max(total, axis=0, keepdims=True))

    peak = lax.fori_loop(0, big // chunk, score, jnp.full((1, total_rows), -jnp.inf, F32))
    summed = jnp.sum(jnp.exp(sc_s[...] - peak), axis=0, keepdims=True)
    st_mine[0:1, :] = peak
    st_mine[1:2, :] = summed
    st_mine[2:8, :] = jnp.zeros((6, total_rows), F32)

    sends = []
    for o in range(1, nd):
        other, dest = peer(o)
        copy = pltpu.make_async_remote_copy(
            src_ref=st_mine, dst_ref=st_all.at[me], send_sem=st_send.at[other], recv_sem=st_recv.at[me],
            device_id=dest, device_id_type=MESH,
        )
        copy.start()
        sends.append(copy)
    st_all[me] = st_mine[...]
    for o in range(1, nd):
        other = lax.rem(me + nd - o, nd)
        pltpu.make_async_remote_copy(
            src_ref=st_mine, dst_ref=st_all.at[other], send_sem=st_send.at[other], recv_sem=st_recv.at[other],
            device_id=partner, device_id_type=MESH,
        ).wait_recv()
    peaks = st_all[:, 0, :]
    top = jnp.max(peaks, axis=0, keepdims=True)
    whole = jnp.sum(st_all[:, 1, :] * jnp.exp(peaks - top), axis=0, keepdims=True)
    logev = top + jnp.log(whole)
    logev_ref[...] = logev
    post_s[...] = jnp.exp(sc_s[...] - logev).astype(BF16)

    def back(first, index_of):
        cols = slice(first, first + 256)
        frame[...] = jnp.dot(post_s[...], s_s[:, cols], preferred_element_type=F32)

        def step(r, carry):
            at = pl.ds(pl.multiple_of(r * kc, kc), kc)
            out = []
            for q in range(2):
                index = jnp.broadcast_to(index_of(q, r), (kc, 128))
                out.append(carry[q] + gather_lanes(frame[at, q * 128 : q * 128 + 128], index))
            return tuple(out)

        zero = jnp.zeros((kc, 128), F32)
        return lax.fori_loop(0, rot, step, (zero, zero))

    left1 = lane((1, 128)) < half
    for j in range(n // 2):
        done = back(j * 256, lambda q, r: inv[2 * j + q, pl.ds(r, 1), :])
        for q in range(2):
            o_mine[2 * j + q, 0:kc, :] = done[q].astype(BF16)
    left_h = lane((kc // 2, 128)) < half
    for j in range(n // 4):
        done = back(
            n * 128 + j * 256,
            lambda q, r: jnp.where(
                left1, inv[4 * j + 2 * q, pl.ds(r, 1), :], inv[4 * j + 2 * q + 1, pl.ds(r, 1), :]
            ),
        )
        for q in range(2):
            low, high = done[q][: kc // 2], done[q][kc // 2 :]
            at = slice(kc, kc + kc // 2)
            o_mine[4 * j + 2 * q, at, :] = jnp.where(left_h, low, pltpu.roll(high, half, 1)).astype(BF16)
            o_mine[4 * j + 2 * q + 1, at, :] = jnp.where(left_h, pltpu.roll(low, half, 1), high).astype(BF16)

    for o in range(1, nd):
        other, dest = peer(o)
        copy = pltpu.make_async_remote_copy(
            src_ref=o_mine.at[dest["shell"]], dst_ref=o_all.at[me], send_sem=o_send.at[other],
            recv_sem=o_recv.at[me], device_id=dest, device_id_type=MESH,
        )
        copy.start()
        sends.append(copy)
    o_all[me] = o_mine[s]
    for o in range(1, nd):
        other = lax.rem(me + nd - o, nd)
        pltpu.make_async_remote_copy(
            src_ref=o_mine.at[0], dst_ref=o_all.at[other], send_sem=o_send.at[other],
            recv_sem=o_recv.at[other], device_id=partner, device_id_type=MESH,
        ).wait_recv()
    for d in range(nd):
        sums_ref[d * kc : d * kc + kc, :] = o_all[d, 0:kc, :].astype(F32)
        packed = o_all[d, kc : kc + kc // 2, :].astype(F32)
        wts_ref[d * kc : d * kc + kc // 2, :] = packed[:, :half]
        wts_ref[d * kc + kc // 2 : d * kc + kc, :] = pltpu.roll(packed, half, 1)[:, :half]
    for copy in copies + relays + sends:
        copy.wait_send()


def fast_body(n, m, particles, classes, ctf, sigma2, shell_of, rot_table, ctf_group):
    width = shell_of.shape[0]
    rot = rot_table.shape[0]
    rows = particles.shape[0]
    k = classes.shape[0]
    groups = ctf.shape[0]
    kc = k // (n * m)
    table = rot_table - lax.axis_index("shell") * width
    spots = jnp.arange(width, dtype=jnp.int32)
    inverse = jnp.sum(
        jnp.where(table[:, :, None] == spots[None, None, :], spots[None, :, None], 0), axis=1
    )
    tabs = jnp.concatenate([table, inverse], axis=1).astype(BF16)
    levels = jnp.arange(sigma2.shape[0], dtype=jnp.int32)
    chosen = jnp.sum(jnp.where(shell_of[:, None] == levels[None, :], sigma2[None, :], 0.0), axis=1)
    weight = 1.0 / chosen
    cw = jnp.concatenate([ctf, jnp.broadcast_to(weight[None, :], ctf.shape)], axis=1)
    lanes = jnp.arange(128, dtype=jnp.int32)
    pick = ((ctf_group[:, None] == (lanes % groups)[None, :]) & (lanes < 3 * groups)[None, :]).astype(BF16)
    total_rows = m * rows
    big = kc * rot
    nd = n * m
    wide = n * 128
    vmem = pl.BlockSpec(memory_space=pltpu.VMEM)
    dma = pltpu.SemaphoreType.DMA
    sums, wts, logev = pl.pallas_call(
        functools.partial(kernel, n, m, kc, rot),
        out_shape=(
            jax.ShapeDtypeStruct((k, 128), F32),
            jax.ShapeDtypeStruct((k, width), F32),
            jax.ShapeDtypeStruct((1, total_rows), F32),
        ),
        in_specs=[vmem] * 5,
        out_specs=(vmem,) * 3,
        scratch_shapes=[
            pltpu.VMEM((m, n, rows, 128), BF16),
            pltpu.VMEM((n, rot, 128), BF16),
            pltpu.VMEM((n, kc, 128), BF16),
            pltpu.VMEM((n, groups, 128), F32),
            pltpu.VMEM((m, rows, 128), BF16),
            pltpu.VMEM((n, rot, 128), jnp.int32),
            pltpu.VMEM((n, rot, 128), jnp.int32),
            pltpu.VMEM((n, kc, 128), F32),
            pltpu.VMEM((total_rows, wide), BF16),
            pltpu.VMEM((total_rows, wide + wide // 2), BF16),
            pltpu.VMEM((4 * groups, wide), BF16),
            pltpu.VMEM((big, wide), BF16),
            pltpu.VMEM((big, wide), BF16),
            pltpu.VMEM((big, wide), BF16),
            pltpu.VMEM((big, total_rows), F32),
            pltpu.VMEM((big, total_rows), BF16),
            pltpu.VMEM((big, 256), F32),
            pltpu.VMEM((8, total_rows), F32),
            pltpu.VMEM((nd, 8, total_rows), F32),
            pltpu.VMEM((n, kc + kc // 2, 128), BF16),
            pltpu.VMEM((nd, kc + kc // 2, 128), BF16),
            dma((4, n)),
            dma((4, n)),
            dma((n,)),
            dma((n,)),
            dma((2,)),
            dma((nd,)),
            dma((nd,)),
            dma((nd,)),
            dma((nd,)),
        ],
        compiler_params=pltpu.CompilerParams(
            collective_id=0, has_side_effects=True, vmem_limit_bytes=48 * 1024 * 1024
        ),
    )(particles, tabs, classes, cw, pick)
    mine = lax.dynamic_slice(logev[0], (lax.axis_index("batch") * rows,), (rows,))
    return sums, wts, mine


def solution(mesh):
    in_specs = (
        P(("groups", "batch"), "shell"),
        P("groups", "shell"),
        P("groups", "shell"),
        P("groups"),
        P("shell"),
        P(None, "shell"),
        P(("groups", "batch")),
    )
    out_specs = (P("groups", "shell"), P("groups", "shell"), P(("groups", "batch")))
    n = mesh.shape["shell"]
    m = mesh.shape["batch"]

    def body(particles, classes, ctf, sigma2, shell_of, rot_table, ctf_group):
        args = (particles, classes, ctf, sigma2, shell_of, rot_table, ctf_group)
        per = classes.shape[0] // (n * m)
        fits = (
            m == 2
            and n % 4 == 0
            and n <= 16
            and classes.shape[0] % (n * m) == 0
            and per % 16 == 0
            and shell_of.shape[0] == 64
            and ctf.shape[0] == 8
            and particles.shape[0] % 16 == 0
            and rot_table.shape[0] % 8 == 0
            and per * rot_table.shape[0] % 128 == 0
        )
        if fits:
            return fast_body(n, m, *args)
        return plain_body(*args)

    return jax.shard_map(body, mesh=mesh, in_specs=in_specs, out_specs=out_specs, check_vma=False)
```

```python
import functools

import jax
import jax.numpy as jnp
from jax import lax
from jax.experimental import pallas as pl
from jax.experimental.pallas import tpu as pltpu
from jax.sharding import PartitionSpec as P

MESH = pl.DeviceIdType.MESH
BF16 = jnp.bfloat16
F32 = jnp.float32


def plain_body(particles, classes, ctf, sigma2, shell_of, rot_table, ctf_group):
    highest = lax.Precision.HIGHEST
    coef_width = shell_of.shape[0]
    class_count = classes.shape[0]
    rotations = rot_table.shape[0]
    levels = sigma2.shape[0]
    group_count = ctf.shape[0]
    offset = lax.axis_index("shell") * coef_width
    local_table = rot_table - offset
    pick_shell = (shell_of[:, None] == jnp.arange(levels, dtype=jnp.int32)[None, :]).astype(F32)
    weight = 1.0 / jnp.dot(pick_shell, sigma2, precision=highest, preferred_element_type=F32)
    pick_group = (ctf_group[:, None] == jnp.arange(group_count, dtype=jnp.int32)[None, :]).astype(F32)
    ctf_part = jnp.dot(pick_group, ctf, precision=highest, preferred_element_type=F32)
    values = particles.astype(F32)
    real_part = values[:, :coef_width]
    imag_part = values[:, coef_width:]
    weighted_ctf = weight[None, :] * ctf_part
    weighted = jnp.concatenate([weighted_ctf * real_part, weighted_ctf * imag_part], axis=1).astype(BF16)
    ctf_power = weight[None, :] * ctf * ctf
    sources = jnp.concatenate(
        [ctf_part * real_part, ctf_part * imag_part, ctf_part * ctf_part], axis=1
    ).astype(BF16)
    class_view = classes.reshape(class_count, 2, coef_width)
    rotated = jnp.take(class_view, local_table, axis=2)
    rotated = jnp.transpose(rotated, (0, 2, 1, 3)).reshape(class_count * rotations, 2 * coef_width)
    cross_terms = lax.dot_general(
        weighted, rotated, (((1,), (1,)), ((), ())), preferred_element_type=F32
    )
    rot_float = rotated.astype(F32)
    class_power = rot_float[:, :coef_width] ** 2 + rot_float[:, coef_width:] ** 2
    penalty = lax.dot_general(
        ctf_power, class_power, (((1,), (1,)), ((), ())), precision=highest, preferred_element_type=F32
    )
    total = lax.psum(
        cross_terms - 0.5 * jnp.dot(pick_group, penalty, precision=highest, preferred_element_type=F32),
        "shell",
    )
    peak = jnp.max(total, axis=1)
    log_evidence = peak + jnp.log(jnp.sum(jnp.exp(total - peak[:, None]), axis=1))
    posterior = jnp.exp(total - log_evidence[:, None]).astype(BF16)
    frames = lax.dot_general(
        posterior, sources, (((0,), (0,)), ((), ())), preferred_element_type=F32
    )
    frames = frames.reshape(class_count, rotations, 3, coef_width)
    placing = (
        local_table[:, :, None] == jnp.arange(coef_width, dtype=jnp.int32)[None, None, :]
    ).astype(F32)
    unrotated = jnp.einsum(
        "krqc,rcd->kqd", frames, placing, precision=highest, preferred_element_type=F32
    )
    sums_part = unrotated[:, 0:2].reshape(class_count, 2 * coef_width)
    weights_part = unrotated[:, 2]
    class_sums, class_weights = lax.psum((sums_part, weights_part), "batch")
    return (class_sums, class_weights, log_evidence)


def split3(x):
    one = x.astype(BF16).astype(F32)
    two = (x - one).astype(BF16).astype(F32)
    return one, two, x - one - two


def gather_lanes(x, index):
    return jnp.take_along_axis(x, index, axis=1, mode="promise_in_bounds")


def kernel(
    n, m, kc, rot, part_ref, tab_ref, cls_ref, cw_ref, pick_ref,
    sums_ref, wts_ref, logev_ref,
    g_part, g_tab, g_cls, g_cw, g_pick, fwd, inv, cls32, w_s, s_s, p_s, r_s, hi_s, lo_s, sc_s, post_s, frame,
    st_mine, st_all, o_mine, o_all,
    in_send, in_recv, relay_send, relay_recv, pick_sem, st_send, st_recv, o_send, o_recv,
):
    s = lax.axis_index("shell")
    b = lax.axis_index("batch")
    rows = part_ref.shape[0]
    total_rows = m * rows
    half = 64
    me = s * m + b
    nd = n * m
    lane = lambda shape: lax.broadcasted_iota(jnp.int32, shape, len(shape) - 1)

    def peer(o):
        other = lax.rem(me + o, nd)
        return other, {"shell": other // m, "batch": lax.rem(other, m)}

    barrier = pltpu.get_barrier_semaphore()
    for o in range(1, nd):
        pl.semaphore_signal(barrier, inc=1, device_id=peer(o)[1], device_id_type=MESH)
    pl.semaphore_wait(barrier, nd - 1)

    copies = []

    def send_in(j, o):
        t = lax.rem(s + o, n)
        first = pl.multiple_of((t * m + b) * kc, kc)
        pairs = (
            (cls_ref.at[pl.ds(first, kc)], g_cls.at[s]),
            (cw_ref, g_cw.at[s]),
            (tab_ref, g_tab.at[s]),
            (part_ref, g_part.at[b, s]),
        )
        copy = pltpu.make_async_remote_copy(
            src_ref=pairs[j][0], dst_ref=pairs[j][1], send_sem=in_send.at[j, t], recv_sem=in_recv.at[j, s],
            device_id={"shell": t, "batch": b}, device_id_type=MESH,
        )
        copy.start()
        copies.append(copy)

    for o in range(1, n):
        for j in range(3):
            send_in(j, o)
    for o in range(1, n):
        send_in(3, o)
    partner = {"shell": s, "batch": 1 - b}
    pick_copy = pltpu.make_async_remote_copy(
        src_ref=pick_ref, dst_ref=g_pick.at[b], send_sem=pick_sem.at[0], recv_sem=pick_sem.at[1],
        device_id=partner, device_id_type=MESH,
    )
    pick_copy.start()
    relays = []

    def relay(src, t):
        copy = pltpu.make_async_remote_copy(
            src_ref=src, dst_ref=g_part.at[b, t], send_sem=relay_send.at[t], recv_sem=relay_recv.at[t],
            device_id=partner, device_id_type=MESH,
        )
        copy.start()
        relays.append(copy)

    relay(part_ref, s)
    g_part[b, s] = part_ref[...]
    g_pick[b] = pick_ref[...]
    g_tab[s] = tab_ref[...]
    g_cw[s] = cw_ref[...]
    g_cls[s] = cls_ref[pl.ds(pl.multiple_of(me * kc, kc), kc), :]

    def arrive(j, t):
        refs = (g_cls.at[t], g_cw.at[t], g_tab.at[t], g_part.at[b, t])
        pltpu.make_async_remote_copy(
            src_ref=refs[j], dst_ref=refs[j], send_sem=in_send.at[j, t], recv_sem=in_recv.at[j, t],
            device_id=partner, device_id_type=MESH,
        ).wait_recv()

    for o in range(1, n):
        t = lax.rem(s + n - o, n)
        arrive(0, t)
        arrive(1, t)
        arrive(2, t)

    left = lane((rot, 128)) < half
    for t in range(n):
        tab = g_tab[t].astype(F32)
        swap = pltpu.roll(tab, half, 1)
        fwd[t] = jnp.where(left, tab, swap + half).astype(jnp.int32)
        inv[t] = jnp.where(left, swap, tab + half).astype(jnp.int32)
        cls32[t] = g_cls[t].astype(F32)

    def rotate(i, carry):
        for u in range(2):
            r = i * 2 + u
            at = pl.ds(pl.multiple_of(r * kc, kc), kc)
            for t in range(n):
                index = jnp.broadcast_to(fwd[t, pl.ds(r, 1), :], (kc, 128))
                turned = gather_lanes(cls32[t], index)
                square = turned * turned
                high = square.astype(BF16)
                cols = slice(t * 128, t * 128 + 128)
                r_s[at, cols] = turned.astype(BF16)
                hi_s[at, cols] = high
                lo_s[at, cols] = (square - high.astype(F32)).astype(BF16)
        return carry

    lax.fori_loop(0, rot // 2, rotate, 0)

    for o in range(1, n):
        t = lax.rem(s + n - o, n)
        arrive(3, t)
        relay(g_part.at[b, t], t)
    pick_copy.wait()
    for o in range(n):
        t = lax.rem(s + o, n)
        pltpu.make_async_remote_copy(
            src_ref=g_part.at[1 - b, t], dst_ref=g_part.at[1 - b, t],
            send_sem=relay_send.at[t], recv_sem=relay_recv.at[t],
            device_id=partner, device_id_type=MESH,
        ).wait_recv()

    pick = g_pick[...].reshape(total_rows, 128)[:, :32]
    left8 = lane((8, 128)) < half
    left_p = lane((total_rows, 128)) < half
    before = None
    for t in range(n):
        packed = g_cw[t]
        swap = pltpu.roll(packed, half, 1)
        ctf = jnp.where(left8, packed, swap)
        weight = jnp.where(left8, swap, packed)
        zero = jnp.zeros_like(ctf)
        pieces = jnp.concatenate(split3(ctf) + (zero,), axis=0).astype(BF16)
        ctf_part = jnp.dot(pick, pieces, preferred_element_type=F32)
        values = g_part[:, t].reshape(total_rows, 128).astype(F32)
        cols = slice(t * 128, t * 128 + 128)
        w_s[:, cols] = (weight[0:1] * ctf_part * values).astype(BF16)
        s_s[:, cols] = (ctf_part * values).astype(BF16)
        p_s[:, cols] = jnp.concatenate(split3(weight * ctf * ctf) + (zero,), axis=0).astype(BF16)
        if t % 2 == 1:
            mixed = jnp.where(left_p, before, ctf_part)
            cols = slice(n * 128 + t // 2 * 128, n * 128 + t // 2 * 128 + 128)
            s_s[:, cols] = (mixed * mixed).astype(BF16)
        before = ctf_part

    nt = (((1,), (1,)), ((), ()))
    chunk = 128
    big = kc * rot

    def score(i, peak):
        at = pl.ds(pl.multiple_of(i * chunk, chunk), chunk)
        cross = lax.dot_general(r_s[at, :], w_s[...], nt, preferred_element_type=F32)
        pen = lax.dot_general(hi_s[at, :], p_s[...], nt, preferred_element_type=F32)
        pen = pen + lax.dot_general(lo_s[at, :], p_s[...], nt, preferred_element_type=F32)
        spread = 0.0
        for piece in split3(pen):
            spread = spread + lax.dot_general(piece.astype(BF16), pick, nt, preferred_element_type=F32)
        total = cross - 0.5 * spread
        sc_s[at, :] = total
        return jnp.maximum(peak, jnp.max(total, axis=0, keepdims=True))

    peak = lax.fori_loop(0, big // chunk, score, jnp.full((1, total_rows), -jnp.inf, F32))
    summed = jnp.sum(jnp.exp(sc_s[...] - peak), axis=0, keepdims=True)
    st_mine[0:1, :] = peak
    st_mine[1:2, :] = summed
    st_mine[2:8, :] = jnp.zeros((6, total_rows), F32)

    sends = []
    for o in range(1, nd):
        other, dest = peer(o)
        copy = pltpu.make_async_remote_copy(
            src_ref=st_mine, dst_ref=st_all.at[me], send_sem=st_send.at[other], recv_sem=st_recv.at[me],
            device_id=dest, device_id_type=MESH,
        )
        copy.start()
        sends.append(copy)
    st_all[me] = st_mine[...]
    for o in range(1, nd):
        other = lax.rem(me + nd - o, nd)
        pltpu.make_async_remote_copy(
            src_ref=st_mine, dst_ref=st_all.at[other], send_sem=st_send.at[other], recv_sem=st_recv.at[other],
            device_id=partner, device_id_type=MESH,
        ).wait_recv()
    peaks = st_all[:, 0, :]
    top = jnp.max(peaks, axis=0, keepdims=True)
    whole = jnp.sum(st_all[:, 1, :] * jnp.exp(peaks - top), axis=0, keepdims=True)
    logev = top + jnp.log(whole)
    logev_ref[...] = logev
    post_s[...] = jnp.exp(sc_s[...] - logev).astype(BF16)

    def back(first, index_of):
        cols = pl.ds(pl.multiple_of(first, 256), 256)
        frame[...] = jnp.dot(post_s[...], s_s[:, cols], preferred_element_type=F32)

        def step(i, carry):
            out = list(carry)
            for u in range(8):
                r = i * 8 + u
                at = pl.ds(pl.multiple_of(r * kc, kc), kc)
                for q in range(2):
                    index = jnp.broadcast_to(index_of(q, r), (kc, 128))
                    out[q] = out[q] + gather_lanes(frame[at, q * 128 : q * 128 + 128], index)
            return tuple(out)

        zero = jnp.zeros((kc, 128), F32)
        return lax.fori_loop(0, rot // 8, step, (zero, zero))

    left1 = lane((1, 128)) < half
    left_h = lane((kc // 2, 128)) < half
    for j in range(n // 4):
        done = back(
            n * 128 + j * 256,
            lambda q, r: jnp.where(
                left1, inv[4 * j + 2 * q, pl.ds(r, 1), :], inv[4 * j + 2 * q + 1, pl.ds(r, 1), :]
            ),
        )
        for q in range(2):
            low, high = done[q][: kc // 2], done[q][kc // 2 :]
            at = slice(kc, kc + kc // 2)
            o_mine[4 * j + 2 * q, at, :] = jnp.where(left_h, low, pltpu.roll(high, half, 1)).astype(BF16)
            o_mine[4 * j + 2 * q + 1, at, :] = jnp.where(left_h, pltpu.roll(low, half, 1), high).astype(BF16)

    def send_out(t, c):
        other = t * m + c
        return pltpu.make_async_remote_copy(
            src_ref=o_mine.at[t], dst_ref=o_all.at[me], send_sem=o_send.at[other],
            recv_sem=o_recv.at[me], device_id={"shell": t, "batch": c}, device_id_type=MESH,
        )

    pairs_of = n // 2
    for j in range(pairs_of):
        base = lax.rem(s // 2 + 1 + j, pairs_of) * 2
        done = back(base * 128, lambda q, r: inv[base + q, pl.ds(r, 1), :])
        for q in range(2):
            o_mine[base + q, 0:kc, :] = done[q].astype(BF16)
        if j < pairs_of - 1:
            for q in range(2):
                for c in range(m):
                    copy = send_out(base + q, c)
                    copy.start()
                    sends.append(copy)
    near = s // 2 * 2 + 1 - lax.rem(s, 2)
    for c in range(m):
        copy = send_out(near, c)
        copy.start()
        sends.append(copy)
    copy = send_out(s, 1 - b)
    copy.start()
    sends.append(copy)
    o_all[me] = o_mine[s]
    for o in range(1, nd):
        other = lax.rem(me + nd - o, nd)
        pltpu.make_async_remote_copy(
            src_ref=o_mine.at[0], dst_ref=o_all.at[other], send_sem=o_send.at[other],
            recv_sem=o_recv.at[other], device_id=partner, device_id_type=MESH,
        ).wait_recv()
    for d in range(nd):
        sums_ref[d * kc : d * kc + kc, :] = o_all[d, 0:kc, :].astype(F32)
        packed = o_all[d, kc : kc + kc // 2, :].astype(F32)
        wts_ref[d * kc : d * kc + kc // 2, :] = packed[:, :half]
        wts_ref[d * kc + kc // 2 : d * kc + kc, :] = pltpu.roll(packed, half, 1)[:, :half]
    for copy in copies + relays + sends:
        copy.wait_send()


def fast_body(n, m, particles, classes, ctf, sigma2, shell_of, rot_table, ctf_group):
    width = shell_of.shape[0]
    rot = rot_table.shape[0]
    rows = particles.shape[0]
    k = classes.shape[0]
    groups = ctf.shape[0]
    kc = k // (n * m)
    table = rot_table - lax.axis_index("shell") * width
    spots = jnp.arange(width, dtype=jnp.int32)
    inverse = jnp.sum(
        jnp.where(table[:, :, None] == spots[None, None, :], spots[None, :, None], 0), axis=1
    )
    tabs = jnp.concatenate([table, inverse], axis=1).astype(BF16)
    levels = jnp.arange(sigma2.shape[0], dtype=jnp.int32)
    chosen = jnp.sum(jnp.where(shell_of[:, None] == levels[None, :], sigma2[None, :], 0.0), axis=1)
    weight = 1.0 / chosen
    cw = jnp.concatenate([ctf, jnp.broadcast_to(weight[None, :], ctf.shape)], axis=1)
    lanes = jnp.arange(128, dtype=jnp.int32)
    pick = ((ctf_group[:, None] == (lanes % groups)[None, :]) & (lanes < 3 * groups)[None, :]).astype(BF16)
    total_rows = m * rows
    big = kc * rot
    nd = n * m
    wide = n * 128
    vmem = pl.BlockSpec(memory_space=pltpu.VMEM)
    dma = pltpu.SemaphoreType.DMA
    sums, wts, logev = pl.pallas_call(
        functools.partial(kernel, n, m, kc, rot),
        out_shape=(
            jax.ShapeDtypeStruct((k, 128), F32),
            jax.ShapeDtypeStruct((k, width), F32),
            jax.ShapeDtypeStruct((1, total_rows), F32),
        ),
        in_specs=[vmem] * 5,
        out_specs=(vmem,) * 3,
        scratch_shapes=[
            pltpu.VMEM((m, n, rows, 128), BF16),
            pltpu.VMEM((n, rot, 128), BF16),
            pltpu.VMEM((n, kc, 128), BF16),
            pltpu.VMEM((n, groups, 128), F32),
            pltpu.VMEM((m, rows, 128), BF16),
            pltpu.VMEM((n, rot, 128), jnp.int32),
            pltpu.VMEM((n, rot, 128), jnp.int32),
            pltpu.VMEM((n, kc, 128), F32),
            pltpu.VMEM((total_rows, wide), BF16),
            pltpu.VMEM((total_rows, wide + wide // 2), BF16),
            pltpu.VMEM((4 * groups, wide), BF16),
            pltpu.VMEM((big, wide), BF16),
            pltpu.VMEM((big, wide), BF16),
            pltpu.VMEM((big, wide), BF16),
            pltpu.VMEM((big, total_rows), F32),
            pltpu.VMEM((big, total_rows), BF16),
            pltpu.VMEM((big, 256), F32),
            pltpu.VMEM((8, total_rows), F32),
            pltpu.VMEM((nd, 8, total_rows), F32),
            pltpu.VMEM((n, kc + kc // 2, 128), BF16),
            pltpu.VMEM((nd, kc + kc // 2, 128), BF16),
            dma((4, n)),
            dma((4, n)),
            dma((n,)),
            dma((n,)),
            dma((2,)),
            dma((nd,)),
            dma((nd,)),
            dma((nd,)),
            dma((nd,)),
        ],
        compiler_params=pltpu.CompilerParams(
            collective_id=0, has_side_effects=True, vmem_limit_bytes=48 * 1024 * 1024
        ),
    )(particles, tabs, classes, cw, pick)
    mine = lax.dynamic_slice(logev[0], (lax.axis_index("batch") * rows,), (rows,))
    return sums, wts, mine


def solution(mesh):
    in_specs = (
        P(("groups", "batch"), "shell"),
        P("groups", "shell"),
        P("groups", "shell"),
        P("groups"),
        P("shell"),
        P(None, "shell"),
        P(("groups", "batch")),
    )
    out_specs = (P("groups", "shell"), P("groups", "shell"), P(("groups", "batch")))
    n = mesh.shape["shell"]
    m = mesh.shape["batch"]

    def body(particles, classes, ctf, sigma2, shell_of, rot_table, ctf_group):
        args = (particles, classes, ctf, sigma2, shell_of, rot_table, ctf_group)
        per = classes.shape[0] // (n * m)
        fits = (
            m == 2
            and n % 4 == 0
            and n <= 16
            and classes.shape[0] % (n * m) == 0
            and per % 16 == 0
            and shell_of.shape[0] == 64
            and ctf.shape[0] == 8
            and particles.shape[0] % 16 == 0
            and rot_table.shape[0] % 16 == 0
            and per * rot_table.shape[0] % 128 == 0
        )
        if fits:
            return fast_body(n, m, *args)
        return plain_body(*args)

    return jax.shard_map(body, mesh=mesh, in_specs=in_specs, out_specs=out_specs, check_vma=False)
```

```python
import functools

import jax
import jax.numpy as jnp
from jax import lax
from jax.experimental import pallas as pl
from jax.experimental.pallas import tpu as pltpu
from jax.sharding import PartitionSpec as P

MESH = pl.DeviceIdType.MESH
BF16 = jnp.bfloat16
F32 = jnp.float32


def plain_body(particles, classes, ctf, sigma2, shell_of, rot_table, ctf_group):
    highest = lax.Precision.HIGHEST
    coef_width = shell_of.shape[0]
    class_count = classes.shape[0]
    rotations = rot_table.shape[0]
    levels = sigma2.shape[0]
    group_count = ctf.shape[0]
    offset = lax.axis_index("shell") * coef_width
    local_table = rot_table - offset
    pick_shell = (shell_of[:, None] == jnp.arange(levels, dtype=jnp.int32)[None, :]).astype(F32)
    weight = 1.0 / jnp.dot(pick_shell, sigma2, precision=highest, preferred_element_type=F32)
    pick_group = (ctf_group[:, None] == jnp.arange(group_count, dtype=jnp.int32)[None, :]).astype(F32)
    ctf_part = jnp.dot(pick_group, ctf, precision=highest, preferred_element_type=F32)
    values = particles.astype(F32)
    real_part = values[:, :coef_width]
    imag_part = values[:, coef_width:]
    weighted_ctf = weight[None, :] * ctf_part
    weighted = jnp.concatenate([weighted_ctf * real_part, weighted_ctf * imag_part], axis=1).astype(BF16)
    ctf_power = weight[None, :] * ctf * ctf
    sources = jnp.concatenate(
        [ctf_part * real_part, ctf_part * imag_part, ctf_part * ctf_part], axis=1
    ).astype(BF16)
    class_view = classes.reshape(class_count, 2, coef_width)
    rotated = jnp.take(class_view, local_table, axis=2)
    rotated = jnp.transpose(rotated, (0, 2, 1, 3)).reshape(class_count * rotations, 2 * coef_width)
    cross_terms = lax.dot_general(
        weighted, rotated, (((1,), (1,)), ((), ())), preferred_element_type=F32
    )
    rot_float = rotated.astype(F32)
    class_power = rot_float[:, :coef_width] ** 2 + rot_float[:, coef_width:] ** 2
    penalty = lax.dot_general(
        ctf_power, class_power, (((1,), (1,)), ((), ())), precision=highest, preferred_element_type=F32
    )
    total = lax.psum(
        cross_terms - 0.5 * jnp.dot(pick_group, penalty, precision=highest, preferred_element_type=F32),
        "shell",
    )
    peak = jnp.max(total, axis=1)
    log_evidence = peak + jnp.log(jnp.sum(jnp.exp(total - peak[:, None]), axis=1))
    posterior = jnp.exp(total - log_evidence[:, None]).astype(BF16)
    frames = lax.dot_general(
        posterior, sources, (((0,), (0,)), ((), ())), preferred_element_type=F32
    )
    frames = frames.reshape(class_count, rotations, 3, coef_width)
    placing = (
        local_table[:, :, None] == jnp.arange(coef_width, dtype=jnp.int32)[None, None, :]
    ).astype(F32)
    unrotated = jnp.einsum(
        "krqc,rcd->kqd", frames, placing, precision=highest, preferred_element_type=F32
    )
    sums_part = unrotated[:, 0:2].reshape(class_count, 2 * coef_width)
    weights_part = unrotated[:, 2]
    class_sums, class_weights = lax.psum((sums_part, weights_part), "batch")
    return (class_sums, class_weights, log_evidence)


def split3(x):
    one = x.astype(BF16).astype(F32)
    two = (x - one).astype(BF16).astype(F32)
    return one, two, x - one - two


def gather_lanes(x, index):
    return jnp.take_along_axis(x, index, axis=1, mode="promise_in_bounds")


def kernel(
    n, m, kc, rot, part_ref, cls_ref, ctf_ref, sigma_ref, shell_ref, table_ref, group_ref,
    sums_ref, wts_ref, logev_ref,
    tab_ref, cw_ref, grp_ref, g_grp, square, w_out, g_part, g_tab, g_cls, g_cw, g_pick, fwd, inv, cls32, w_s, s_s, p_s, r_s, hi_s, lo_s, sc_s, post_s, frame,
    st_mine, st_all, o_mine, o_all,
    in_send, in_recv, relay_send, relay_recv, pick_sem, st_send, st_recv, o_send, o_recv,
):
    s = lax.axis_index("shell")
    b = lax.axis_index("batch")
    rows = part_ref.shape[0]
    total_rows = m * rows
    half = 64
    me = s * m + b
    nd = n * m
    lane = lambda shape: lax.broadcasted_iota(jnp.int32, shape, len(shape) - 1)

    def peer(o):
        other = lax.rem(me + o, nd)
        return other, {"shell": other // m, "batch": lax.rem(other, m)}

    barrier = pltpu.get_barrier_semaphore()
    for o in range(1, nd):
        pl.semaphore_signal(barrier, inc=1, device_id=peer(o)[1], device_id_type=MESH)

    def sub(shape):
        return lax.broadcasted_iota(jnp.int32, shape, 0)

    table = (table_ref[...] - s * half).astype(F32)
    table = jnp.concatenate([table, jnp.zeros_like(table)], axis=1)
    tall = jnp.concatenate([table, jnp.zeros((128 - rot, 128), F32)], axis=0)
    square[...] = tall.T
    spots = sub((half, 128)).astype(F32)
    found = jnp.zeros((half, 128), F32)
    for c in range(half):
        found = jnp.where(square[c : c + 1, :] == spots, float(c), found)
    back_table = jnp.concatenate([found, jnp.zeros_like(found)], axis=0).T[:rot]
    tab_ref[...] = (table + pltpu.roll(back_table, half, 1)).astype(BF16)
    levels = sigma_ref.shape[1]
    chosen_level = (shell_ref[...] == sub((levels, half))).astype(F32).astype(BF16)
    one, two, three = split3(sigma_ref[...])
    order = sub((8, levels))
    stack = jnp.where(order == 0, one, jnp.where(order == 1, two, jnp.where(order == 2, three, 0.0)))
    chosen = jnp.dot(stack.astype(BF16), chosen_level, preferred_element_type=F32)
    weight = 1.0 / jnp.sum(chosen, axis=0, keepdims=True)
    ctf = ctf_ref[...]
    cw_ref[...] = jnp.concatenate([ctf, jnp.broadcast_to(weight, ctf.shape)], axis=1)
    grp_ref[...] = jnp.zeros_like(grp_ref)
    grp_ref[:, :rows] = group_ref[...]

    pl.semaphore_wait(barrier, nd - 1)

    copies = []

    def send_in(j, o):
        t = lax.rem(s + o, n)
        first = pl.multiple_of((t * m + b) * kc, kc)
        pairs = (
            (cls_ref.at[pl.ds(first, kc)], g_cls.at[s]),
            (cw_ref, g_cw.at[s]),
            (tab_ref, g_tab.at[s]),
            (part_ref, g_part.at[b, s]),
        )
        copy = pltpu.make_async_remote_copy(
            src_ref=pairs[j][0], dst_ref=pairs[j][1], send_sem=in_send.at[j, t], recv_sem=in_recv.at[j, s],
            device_id={"shell": t, "batch": b}, device_id_type=MESH,
        )
        copy.start()
        copies.append(copy)

    for o in range(1, n):
        for j in range(3):
            send_in(j, o)
    for o in range(1, n):
        send_in(3, o)
    partner = {"shell": s, "batch": 1 - b}
    pick_copy = pltpu.make_async_remote_copy(
        src_ref=grp_ref, dst_ref=g_grp.at[b], send_sem=pick_sem.at[0], recv_sem=pick_sem.at[1],
        device_id=partner, device_id_type=MESH,
    )
    pick_copy.start()
    relays = []

    def relay(src, t):
        copy = pltpu.make_async_remote_copy(
            src_ref=src, dst_ref=g_part.at[b, t], send_sem=relay_send.at[t], recv_sem=relay_recv.at[t],
            device_id=partner, device_id_type=MESH,
        )
        copy.start()
        relays.append(copy)

    relay(part_ref, s)
    g_part[b, s] = part_ref[...]
    g_grp[b] = grp_ref[...]
    g_tab[s] = tab_ref[...]
    g_cw[s] = cw_ref[...]
    g_cls[s] = cls_ref[pl.ds(pl.multiple_of(me * kc, kc), kc), :]

    def arrive(j, t):
        refs = (g_cls.at[t], g_cw.at[t], g_tab.at[t], g_part.at[b, t])
        pltpu.make_async_remote_copy(
            src_ref=refs[j], dst_ref=refs[j], send_sem=in_send.at[j, t], recv_sem=in_recv.at[j, t],
            device_id=partner, device_id_type=MESH,
        ).wait_recv()

    for o in range(1, n):
        t = lax.rem(s + n - o, n)
        arrive(0, t)
        arrive(1, t)
        arrive(2, t)

    left = lane((rot, 128)) < half
    for t in range(n):
        tab = g_tab[t].astype(F32)
        swap = pltpu.roll(tab, half, 1)
        fwd[t] = jnp.where(left, tab, swap + half).astype(jnp.int32)
        inv[t] = jnp.where(left, swap, tab + half).astype(jnp.int32)
        cls32[t] = g_cls[t].astype(F32)

    def rotate(i, carry):
        for u in range(2):
            r = i * 2 + u
            at = pl.ds(pl.multiple_of(r * kc, kc), kc)
            for t in range(n):
                index = jnp.broadcast_to(fwd[t, pl.ds(r, 1), :], (kc, 128))
                turned = gather_lanes(cls32[t], index)
                power = turned * turned
                high = power.astype(BF16)
                cols = slice(t * 128, t * 128 + 128)
                r_s[at, cols] = turned.astype(BF16)
                hi_s[at, cols] = high
                lo_s[at, cols] = (power - high.astype(F32)).astype(BF16)
        return carry

    lax.fori_loop(0, rot // 2, rotate, 0)

    for o in range(1, n):
        t = lax.rem(s + n - o, n)
        arrive(3, t)
        relay(g_part.at[b, t], t)
    pick_copy.wait()
    place = sub((128, 128))
    for c in range(m):
        member = (g_grp[c] == (place & 7)) & (place < 24)
        g_pick[c] = member.astype(F32).T[:rows].astype(BF16)
    for o in range(n):
        t = lax.rem(s + o, n)
        pltpu.make_async_remote_copy(
            src_ref=g_part.at[1 - b, t], dst_ref=g_part.at[1 - b, t],
            send_sem=relay_send.at[t], recv_sem=relay_recv.at[t],
            device_id=partner, device_id_type=MESH,
        ).wait_recv()

    pick = g_pick[...].reshape(total_rows, 128)[:, :32]
    left8 = lane((8, 128)) < half
    left_p = lane((total_rows, 128)) < half
    before = None
    for t in range(n):
        packed = g_cw[t]
        swap = pltpu.roll(packed, half, 1)
        ctf = jnp.where(left8, packed, swap)
        weight = jnp.where(left8, swap, packed)
        zero = jnp.zeros_like(ctf)
        pieces = jnp.concatenate(split3(ctf) + (zero,), axis=0).astype(BF16)
        ctf_part = jnp.dot(pick, pieces, preferred_element_type=F32)
        values = g_part[:, t].reshape(total_rows, 128).astype(F32)
        cols = slice(t * 128, t * 128 + 128)
        w_s[:, cols] = (weight[0:1] * ctf_part * values).astype(BF16)
        s_s[:, cols] = (ctf_part * values).astype(BF16)
        p_s[:, cols] = jnp.concatenate(split3(weight * ctf * ctf) + (zero,), axis=0).astype(BF16)
        if t % 2 == 1:
            mixed = jnp.where(left_p, before, ctf_part)
            cols = slice(n * 128 + t // 2 * 128, n * 128 + t // 2 * 128 + 128)
            s_s[:, cols] = (mixed * mixed).astype(BF16)
        before = ctf_part

    nt = (((1,), (1,)), ((), ()))
    chunk = 128
    big = kc * rot

    def score(i, peak):
        at = pl.ds(pl.multiple_of(i * chunk, chunk), chunk)
        cross = lax.dot_general(r_s[at, :], w_s[...], nt, preferred_element_type=F32)
        pen = lax.dot_general(hi_s[at, :], p_s[...], nt, preferred_element_type=F32)
        pen = pen + lax.dot_general(lo_s[at, :], p_s[...], nt, preferred_element_type=F32)
        spread = 0.0
        for piece in split3(pen):
            spread = spread + lax.dot_general(piece.astype(BF16), pick, nt, preferred_element_type=F32)
        total = cross - 0.5 * spread
        sc_s[at, :] = total
        return jnp.maximum(peak, jnp.max(total, axis=0, keepdims=True))

    peak = lax.fori_loop(0, big // chunk, score, jnp.full((1, total_rows), -jnp.inf, F32))
    summed = jnp.sum(jnp.exp(sc_s[...] - peak), axis=0, keepdims=True)
    st_mine[0:1, :] = peak
    st_mine[1:2, :] = summed
    st_mine[2:8, :] = jnp.zeros((6, total_rows), F32)

    sends = []
    for o in range(1, nd):
        other, dest = peer(o)
        copy = pltpu.make_async_remote_copy(
            src_ref=st_mine, dst_ref=st_all.at[me], send_sem=st_send.at[other], recv_sem=st_recv.at[me],
            device_id=dest, device_id_type=MESH,
        )
        copy.start()
        sends.append(copy)
    st_all[me] = st_mine[...]
    for o in range(1, nd):
        other = lax.rem(me + nd - o, nd)
        pltpu.make_async_remote_copy(
            src_ref=st_mine, dst_ref=st_all.at[other], send_sem=st_send.at[other], recv_sem=st_recv.at[other],
            device_id=partner, device_id_type=MESH,
        ).wait_recv()
    peaks = st_all[:, 0, :]
    top = jnp.max(peaks, axis=0, keepdims=True)
    whole = jnp.sum(st_all[:, 1, :] * jnp.exp(peaks - top), axis=0, keepdims=True)
    logev = top + jnp.log(whole)
    logev_ref[...] = jnp.where(b == 0, logev[:, :rows], logev[:, rows:])
    post_s[...] = jnp.exp(sc_s[...] - logev).astype(BF16)

    def back(first, index_of):
        cols = pl.ds(pl.multiple_of(first, 256), 256)
        frame[...] = jnp.dot(post_s[...], s_s[:, cols], preferred_element_type=F32)

        def step(i, carry):
            out = list(carry)
            for u in range(8):
                r = i * 8 + u
                at = pl.ds(pl.multiple_of(r * kc, kc), kc)
                for q in range(2):
                    index = jnp.broadcast_to(index_of(q, r), (kc, 128))
                    out[q] = out[q] + gather_lanes(frame[at, q * 128 : q * 128 + 128], index)
            return tuple(out)

        zero = jnp.zeros((kc, 128), F32)
        return lax.fori_loop(0, rot // 8, step, (zero, zero))

    left1 = lane((1, 128)) < half
    left_h = lane((kc // 2, 128)) < half
    for j in range(n // 4):
        done = back(
            n * 128 + j * 256,
            lambda q, r: jnp.where(
                left1, inv[4 * j + 2 * q, pl.ds(r, 1), :], inv[4 * j + 2 * q + 1, pl.ds(r, 1), :]
            ),
        )
        for q in range(2):
            low, high = done[q][: kc // 2], done[q][kc // 2 :]
            at = slice(kc, kc + kc // 2)
            o_mine[4 * j + 2 * q, at, :] = jnp.where(left_h, low, pltpu.roll(high, half, 1)).astype(BF16)
            o_mine[4 * j + 2 * q + 1, at, :] = jnp.where(left_h, pltpu.roll(low, half, 1), high).astype(BF16)

    def send_out(t, c):
        other = t * m + c
        return pltpu.make_async_remote_copy(
            src_ref=o_mine.at[t], dst_ref=o_all.at[me], send_sem=o_send.at[other],
            recv_sem=o_recv.at[me], device_id={"shell": t, "batch": c}, device_id_type=MESH,
        )

    pairs_of = n // 2
    for j in range(pairs_of):
        base = lax.rem(s // 2 + 1 + j, pairs_of) * 2
        done = back(base * 128, lambda q, r: inv[base + q, pl.ds(r, 1), :])
        for q in range(2):
            o_mine[base + q, 0:kc, :] = done[q].astype(BF16)
        if j < pairs_of - 1:
            for q in range(2):
                for c in range(m):
                    copy = send_out(base + q, c)
                    copy.start()
                    sends.append(copy)
    near = s // 2 * 2 + 1 - lax.rem(s, 2)
    for c in range(m):
        copy = send_out(near, c)
        copy.start()
        sends.append(copy)
    copy = send_out(s, 1 - b)
    copy.start()
    sends.append(copy)
    o_all[me] = o_mine[s]
    for o in range(1, nd):
        other = lax.rem(me + nd - o, nd)
        pltpu.make_async_remote_copy(
            src_ref=o_mine.at[0], dst_ref=o_all.at[other], send_sem=o_send.at[other],
            recv_sem=o_recv.at[other], device_id=partner, device_id_type=MESH,
        ).wait_recv()
    for d in range(nd):
        sums_ref[d * kc : d * kc + kc, :] = o_all[d, 0:kc, :].astype(F32)
        packed = o_all[d, kc : kc + kc // 2, :].astype(F32)
        w_out[d * kc : d * kc + kc // 2, :] = packed
        w_out[d * kc + kc // 2 : d * kc + kc, :] = pltpu.roll(packed, half, 1)
    for d in range(nd * kc // 128):
        wts_ref[:, d * 128 : d * 128 + 128] = w_out[d * 128 : d * 128 + 128, :].T[:half]
    for copy in copies + relays + sends:
        copy.wait_send()


def fast_body(n, m, particles, classes, ctf, sigma2, shell_of, rot_table, ctf_group):
    width = shell_of.shape[0]
    rot = rot_table.shape[0]
    rows = particles.shape[0]
    k = classes.shape[0]
    groups = ctf.shape[0]
    kc = k // (n * m)
    total_rows = m * rows
    big = kc * rot
    nd = n * m
    wide = n * 128
    vmem = pl.BlockSpec(memory_space=pltpu.VMEM)
    dma = pltpu.SemaphoreType.DMA
    sums, wts, logev = pl.pallas_call(
        functools.partial(kernel, n, m, kc, rot),
        out_shape=(
            jax.ShapeDtypeStruct((k, 128), F32),
            jax.ShapeDtypeStruct((width, k), F32),
            jax.ShapeDtypeStruct((1, rows), F32),
        ),
        in_specs=[vmem] * 7,
        out_specs=(vmem,) * 3,
        scratch_shapes=[
            pltpu.VMEM((rot, 128), BF16),
            pltpu.VMEM((groups, 128), F32),
            pltpu.VMEM((1, 128), jnp.int32),
            pltpu.VMEM((m, 1, 128), jnp.int32),
            pltpu.VMEM((128, 128), F32),
            pltpu.VMEM((k, 128), F32),
            pltpu.VMEM((m, n, rows, 128), BF16),
            pltpu.VMEM((n, rot, 128), BF16),
            pltpu.VMEM((n, kc, 128), BF16),
            pltpu.VMEM((n, groups, 128), F32),
            pltpu.VMEM((m, rows, 128), BF16),
            pltpu.VMEM((n, rot, 128), jnp.int32),
            pltpu.VMEM((n, rot, 128), jnp.int32),
            pltpu.VMEM((n, kc, 128), F32),
            pltpu.VMEM((total_rows, wide), BF16),
            pltpu.VMEM((total_rows, wide + wide // 2), BF16),
            pltpu.VMEM((4 * groups, wide), BF16),
            pltpu.VMEM((big, wide), BF16),
            pltpu.VMEM((big, wide), BF16),
            pltpu.VMEM((big, wide), BF16),
            pltpu.VMEM((big, total_rows), F32),
            pltpu.VMEM((big, total_rows), BF16),
            pltpu.VMEM((big, 256), F32),
            pltpu.VMEM((8, total_rows), F32),
            pltpu.VMEM((nd, 8, total_rows), F32),
            pltpu.VMEM((n, kc + kc // 2, 128), BF16),
            pltpu.VMEM((nd, kc + kc // 2, 128), BF16),
            dma((4, n)),
            dma((4, n)),
            dma((n,)),
            dma((n,)),
            dma((2,)),
            dma((nd,)),
            dma((nd,)),
            dma((nd,)),
            dma((nd,)),
        ],
        compiler_params=pltpu.CompilerParams(
            collective_id=0, has_side_effects=True, vmem_limit_bytes=48 * 1024 * 1024
        ),
    )(particles, classes, ctf, sigma2[None, :], shell_of[None, :], rot_table, ctf_group[None, :])
    return sums, wts.T, logev[0]


def solution(mesh):
    in_specs = (
        P(("groups", "batch"), "shell"),
        P("groups", "shell"),
        P("groups", "shell"),
        P("groups"),
        P("shell"),
        P(None, "shell"),
        P(("groups", "batch")),
    )
    out_specs = (P("groups", "shell"), P("groups", "shell"), P(("groups", "batch")))
    n = mesh.shape["shell"]
    m = mesh.shape["batch"]

    def body(particles, classes, ctf, sigma2, shell_of, rot_table, ctf_group):
        args = (particles, classes, ctf, sigma2, shell_of, rot_table, ctf_group)
        per = classes.shape[0] // (n * m)
        fits = (
            m == 2
            and n % 4 == 0
            and n <= 16
            and classes.shape[0] % (n * m) == 0
            and per % 16 == 0
            and shell_of.shape[0] == 64
            and ctf.shape[0] == 8
            and particles.shape[0] % 16 == 0
            and particles.shape[0] <= 128
            and rot_table.shape[0] <= 128
            and classes.shape[0] % 128 == 0
            and sigma2.shape[0] % 8 == 0
            and rot_table.shape[0] % 16 == 0
            and per * rot_table.shape[0] % 128 == 0
        )
        if fits:
            return fast_body(n, m, *args)
        return plain_body(*args)

    return jax.shard_map(body, mesh=mesh, in_specs=in_specs, out_specs=out_specs, check_vma=False)
```

```python
import functools

import jax
import jax.numpy as jnp
from jax import lax
from jax.experimental import pallas as pl
from jax.experimental.pallas import tpu as pltpu
from jax.sharding import PartitionSpec as P

MESH = pl.DeviceIdType.MESH
BF16 = jnp.bfloat16
F32 = jnp.float32


def plain_body(particles, classes, ctf, sigma2, shell_of, rot_table, ctf_group):
    highest = lax.Precision.HIGHEST
    coef_width = shell_of.shape[0]
    class_count = classes.shape[0]
    rotations = rot_table.shape[0]
    levels = sigma2.shape[0]
    group_count = ctf.shape[0]
    offset = lax.axis_index("shell") * coef_width
    local_table = rot_table - offset
    pick_shell = (shell_of[:, None] == jnp.arange(levels, dtype=jnp.int32)[None, :]).astype(F32)
    weight = 1.0 / jnp.dot(pick_shell, sigma2, precision=highest, preferred_element_type=F32)
    pick_group = (ctf_group[:, None] == jnp.arange(group_count, dtype=jnp.int32)[None, :]).astype(F32)
    ctf_part = jnp.dot(pick_group, ctf, precision=highest, preferred_element_type=F32)
    values = particles.astype(F32)
    real_part = values[:, :coef_width]
    imag_part = values[:, coef_width:]
    weighted_ctf = weight[None, :] * ctf_part
    weighted = jnp.concatenate([weighted_ctf * real_part, weighted_ctf * imag_part], axis=1).astype(BF16)
    ctf_power = weight[None, :] * ctf * ctf
    sources = jnp.concatenate(
        [ctf_part * real_part, ctf_part * imag_part, ctf_part * ctf_part], axis=1
    ).astype(BF16)
    class_view = classes.reshape(class_count, 2, coef_width)
    rotated = jnp.take(class_view, local_table, axis=2)
    rotated = jnp.transpose(rotated, (0, 2, 1, 3)).reshape(class_count * rotations, 2 * coef_width)
    cross_terms = lax.dot_general(
        weighted, rotated, (((1,), (1,)), ((), ())), preferred_element_type=F32
    )
    rot_float = rotated.astype(F32)
    class_power = rot_float[:, :coef_width] ** 2 + rot_float[:, coef_width:] ** 2
    penalty = lax.dot_general(
        ctf_power, class_power, (((1,), (1,)), ((), ())), precision=highest, preferred_element_type=F32
    )
    total = lax.psum(
        cross_terms - 0.5 * jnp.dot(pick_group, penalty, precision=highest, preferred_element_type=F32),
        "shell",
    )
    peak = jnp.max(total, axis=1)
    log_evidence = peak + jnp.log(jnp.sum(jnp.exp(total - peak[:, None]), axis=1))
    posterior = jnp.exp(total - log_evidence[:, None]).astype(BF16)
    frames = lax.dot_general(
        posterior, sources, (((0,), (0,)), ((), ())), preferred_element_type=F32
    )
    frames = frames.reshape(class_count, rotations, 3, coef_width)
    placing = (
        local_table[:, :, None] == jnp.arange(coef_width, dtype=jnp.int32)[None, None, :]
    ).astype(F32)
    unrotated = jnp.einsum(
        "krqc,rcd->kqd", frames, placing, precision=highest, preferred_element_type=F32
    )
    sums_part = unrotated[:, 0:2].reshape(class_count, 2 * coef_width)
    weights_part = unrotated[:, 2]
    class_sums, class_weights = lax.psum((sums_part, weights_part), "batch")
    return (class_sums, class_weights, log_evidence)


def split3(x):
    one = x.astype(BF16).astype(F32)
    two = (x - one).astype(BF16).astype(F32)
    return one, two, x - one - two


def gather_lanes(x, index):
    return jnp.take_along_axis(x, index, axis=1, mode="promise_in_bounds")


def kernel(
    n, m, kc, rot, part_in, cls_in, ctf_in, sigma_in, shell_in, table_in, group_in,
    sums_ref, wts_ref, logev_ref,
    part_ref, cls_ref, ctf_ref, sigma_ref, shell_ref, table_ref, group_ref, load_sem,
    tab_ref, cw_ref, grp_ref, g_grp, square, w_out, g_part, g_tab, g_cls, g_cw, g_pick, fwd, inv, cls32, w_s, s_s, p_s, r_s, hi_s, lo_s, sc_s, post_s, frame,
    st_mine, st_all, o_mine, o_all,
    in_send, in_recv, relay_send, relay_recv, pick_sem, st_send, st_recv, o_send, o_recv,
):
    s = lax.axis_index("shell")
    b = lax.axis_index("batch")
    rows = part_ref.shape[0]
    total_rows = m * rows
    half = 64
    me = s * m + b
    nd = n * m
    lane = lambda shape: lax.broadcasted_iota(jnp.int32, shape, len(shape) - 1)

    def peer(o):
        other = lax.rem(me + o, nd)
        return other, {"shell": other // m, "batch": lax.rem(other, m)}

    loads = [
        pltpu.make_async_copy(src, dst, load_sem.at[j])
        for j, (src, dst) in enumerate(
            (
                (table_in, table_ref), (sigma_in, sigma_ref), (shell_in, shell_ref), (ctf_in, ctf_ref),
                (group_in, group_ref), (cls_in, cls_ref), (part_in, part_ref),
            )
        )
    ]
    for load in loads:
        load.start()
    barrier = pltpu.get_barrier_semaphore()
    for o in range(1, nd):
        pl.semaphore_signal(barrier, inc=1, device_id=peer(o)[1], device_id_type=MESH)

    def sub(shape):
        return lax.broadcasted_iota(jnp.int32, shape, 0)

    for load in loads:
        load.wait()
    table = (table_ref[...] - s * half).astype(F32)
    table = jnp.concatenate([table, jnp.zeros_like(table)], axis=1)
    tall = jnp.concatenate([table, jnp.zeros((128 - rot, 128), F32)], axis=0)
    square[...] = tall.T
    spots = sub((half, 128)).astype(F32)
    found = jnp.zeros((half, 128), F32)
    for c in range(half):
        found = jnp.where(square[c : c + 1, :] == spots, float(c), found)
    back_table = jnp.concatenate([found, jnp.zeros_like(found)], axis=0).T[:rot]
    tab_ref[...] = (table + pltpu.roll(back_table, half, 1)).astype(BF16)
    levels = sigma_ref.shape[1]
    chosen_level = (shell_ref[...] == sub((levels, half))).astype(F32).astype(BF16)
    one, two, three = split3(sigma_ref[...])
    order = sub((8, levels))
    stack = jnp.where(order == 0, one, jnp.where(order == 1, two, jnp.where(order == 2, three, 0.0)))
    chosen = jnp.dot(stack.astype(BF16), chosen_level, preferred_element_type=F32)
    weight = 1.0 / jnp.sum(chosen, axis=0, keepdims=True)
    ctf = ctf_ref[...]
    cw_ref[...] = jnp.concatenate([ctf, jnp.broadcast_to(weight, ctf.shape)], axis=1)
    grp_ref[...] = jnp.zeros_like(grp_ref)
    grp_ref[:, :rows] = group_ref[...]

    pl.semaphore_wait(barrier, nd - 1)

    copies = []

    def send_in(j, o):
        t = lax.rem(s + o, n)
        first = pl.multiple_of((t * m + b) * kc, kc)
        pairs = (
            (cls_ref.at[pl.ds(first, kc)], g_cls.at[s]),
            (cw_ref, g_cw.at[s]),
            (tab_ref, g_tab.at[s]),
            (part_ref, g_part.at[b, s]),
        )
        copy = pltpu.make_async_remote_copy(
            src_ref=pairs[j][0], dst_ref=pairs[j][1], send_sem=in_send.at[j, t], recv_sem=in_recv.at[j, s],
            device_id={"shell": t, "batch": b}, device_id_type=MESH,
        )
        copy.start()
        copies.append(copy)

    for o in range(1, n):
        for j in range(3):
            send_in(j, o)
    for o in range(1, n):
        send_in(3, o)
    partner = {"shell": s, "batch": 1 - b}
    pick_copy = pltpu.make_async_remote_copy(
        src_ref=grp_ref, dst_ref=g_grp.at[b], send_sem=pick_sem.at[0], recv_sem=pick_sem.at[1],
        device_id=partner, device_id_type=MESH,
    )
    pick_copy.start()
    relays = []

    def relay(src, t):
        copy = pltpu.make_async_remote_copy(
            src_ref=src, dst_ref=g_part.at[b, t], send_sem=relay_send.at[t], recv_sem=relay_recv.at[t],
            device_id=partner, device_id_type=MESH,
        )
        copy.start()
        relays.append(copy)

    relay(part_ref, s)
    g_part[b, s] = part_ref[...]
    g_grp[b] = grp_ref[...]
    g_tab[s] = tab_ref[...]
    g_cw[s] = cw_ref[...]
    g_cls[s] = cls_ref[pl.ds(pl.multiple_of(me * kc, kc), kc), :]

    def arrive(j, t):
        refs = (g_cls.at[t], g_cw.at[t], g_tab.at[t], g_part.at[b, t])
        pltpu.make_async_remote_copy(
            src_ref=refs[j], dst_ref=refs[j], send_sem=in_send.at[j, t], recv_sem=in_recv.at[j, t],
            device_id=partner, device_id_type=MESH,
        ).wait_recv()

    for o in range(1, n):
        t = lax.rem(s + n - o, n)
        arrive(0, t)
        arrive(1, t)
        arrive(2, t)

    left = lane((rot, 128)) < half
    for t in range(n):
        tab = g_tab[t].astype(F32)
        swap = pltpu.roll(tab, half, 1)
        fwd[t] = jnp.where(left, tab, swap + half).astype(jnp.int32)
        inv[t] = jnp.where(left, swap, tab + half).astype(jnp.int32)
        cls32[t] = g_cls[t].astype(F32)

    def rotate(i, carry):
        for u in range(4):
            r = i * 4 + u
            at = pl.ds(pl.multiple_of(r * kc, kc), kc)
            for t in range(n):
                index = jnp.broadcast_to(fwd[t, pl.ds(r, 1), :], (kc, 128))
                turned = gather_lanes(cls32[t], index)
                power = turned * turned
                high = power.astype(BF16)
                cols = slice(t * 128, t * 128 + 128)
                r_s[at, cols] = turned.astype(BF16)
                hi_s[at, cols] = high
                lo_s[at, cols] = (power - high.astype(F32)).astype(BF16)
        return carry

    lax.fori_loop(0, rot // 4, rotate, 0)

    for o in range(1, n):
        t = lax.rem(s + n - o, n)
        arrive(3, t)
        relay(g_part.at[b, t], t)
    pick_copy.wait()
    place = sub((128, 128))
    for c in range(m):
        member = (g_grp[c] == (place & 7)) & (place < 24)
        g_pick[c] = member.astype(F32).T[:rows].astype(BF16)
    for o in range(n):
        t = lax.rem(s + o, n)
        pltpu.make_async_remote_copy(
            src_ref=g_part.at[1 - b, t], dst_ref=g_part.at[1 - b, t],
            send_sem=relay_send.at[t], recv_sem=relay_recv.at[t],
            device_id=partner, device_id_type=MESH,
        ).wait_recv()

    pick = g_pick[...].reshape(total_rows, 128)[:, :32]
    left8 = lane((8, 128)) < half
    left_p = lane((total_rows, 128)) < half
    before = None
    for t in range(n):
        packed = g_cw[t]
        swap = pltpu.roll(packed, half, 1)
        ctf = jnp.where(left8, packed, swap)
        weight = jnp.where(left8, swap, packed)
        zero = jnp.zeros_like(ctf)
        pieces = jnp.concatenate(split3(ctf) + (zero,), axis=0).astype(BF16)
        ctf_part = jnp.dot(pick, pieces, preferred_element_type=F32)
        values = g_part[:, t].reshape(total_rows, 128).astype(F32)
        cols = slice(t * 128, t * 128 + 128)
        w_s[:, cols] = (weight[0:1] * ctf_part * values).astype(BF16)
        s_s[:, cols] = (ctf_part * values).astype(BF16)
        p_s[:, cols] = jnp.concatenate(split3(weight * ctf * ctf) + (zero,), axis=0).astype(BF16)
        if t % 2 == 1:
            mixed = jnp.where(left_p, before, ctf_part)
            cols = slice(n * 128 + t // 2 * 128, n * 128 + t // 2 * 128 + 128)
            s_s[:, cols] = (mixed * mixed).astype(BF16)
        before = ctf_part

    nt = (((1,), (1,)), ((), ()))
    chunk = 384
    big = kc * rot

    def score(i, peak):
        at = pl.ds(pl.multiple_of(i * chunk, chunk), chunk)
        cross = lax.dot_general(r_s[at, :], w_s[...], nt, preferred_element_type=F32)
        pen = lax.dot_general(hi_s[at, :], p_s[...], nt, preferred_element_type=F32)
        pen = pen + lax.dot_general(lo_s[at, :], p_s[...], nt, preferred_element_type=F32)
        spread = 0.0
        for piece in split3(pen):
            spread = spread + lax.dot_general(piece.astype(BF16), pick, nt, preferred_element_type=F32)
        total = cross - 0.5 * spread
        sc_s[at, :] = total
        return jnp.maximum(peak, jnp.max(total, axis=0, keepdims=True))

    peak = lax.fori_loop(0, big // chunk, score, jnp.full((1, total_rows), -jnp.inf, F32))
    summed = jnp.sum(jnp.exp(sc_s[...] - peak), axis=0, keepdims=True)
    st_mine[0:1, :] = peak
    st_mine[1:2, :] = summed
    st_mine[2:8, :] = jnp.zeros((6, total_rows), F32)

    sends = []
    for o in range(1, nd):
        other, dest = peer(o)
        copy = pltpu.make_async_remote_copy(
            src_ref=st_mine, dst_ref=st_all.at[me], send_sem=st_send.at[other], recv_sem=st_recv.at[me],
            device_id=dest, device_id_type=MESH,
        )
        copy.start()
        sends.append(copy)
    st_all[me] = st_mine[...]
    for o in range(1, nd):
        other = lax.rem(me + nd - o, nd)
        pltpu.make_async_remote_copy(
            src_ref=st_mine, dst_ref=st_all.at[other], send_sem=st_send.at[other], recv_sem=st_recv.at[other],
            device_id=partner, device_id_type=MESH,
        ).wait_recv()
    peaks = st_all[:, 0, :]
    top = jnp.max(peaks, axis=0, keepdims=True)
    whole = jnp.sum(st_all[:, 1, :] * jnp.exp(peaks - top), axis=0, keepdims=True)
    logev = top + jnp.log(whole)
    logev_ref[...] = jnp.where(b == 0, logev[:, :rows], logev[:, rows:])
    post_s[...] = jnp.exp(sc_s[...] - logev).astype(BF16)

    def back(first, index_of):
        cols = pl.ds(pl.multiple_of(first, 256), 256)
        frame[...] = jnp.dot(post_s[...], s_s[:, cols], preferred_element_type=F32)

        def step(i, carry):
            out = list(carry)
            for u in range(24):
                r = i * 24 + u
                at = pl.ds(pl.multiple_of(r * kc, kc), kc)
                for q in range(2):
                    index = jnp.broadcast_to(index_of(q, r), (kc, 128))
                    out[q] = out[q] + gather_lanes(frame[at, q * 128 : q * 128 + 128], index)
            return tuple(out)

        zero = jnp.zeros((kc, 128), F32)
        return lax.fori_loop(0, rot // 24, step, (zero, zero))

    left1 = lane((1, 128)) < half
    left_h = lane((kc // 2, 128)) < half
    for j in range(n // 4):
        done = back(
            n * 128 + j * 256,
            lambda q, r: jnp.where(
                left1, inv[4 * j + 2 * q, pl.ds(r, 1), :], inv[4 * j + 2 * q + 1, pl.ds(r, 1), :]
            ),
        )
        for q in range(2):
            low, high = done[q][: kc // 2], done[q][kc // 2 :]
            at = slice(kc, kc + kc // 2)
            o_mine[4 * j + 2 * q, at, :] = jnp.where(left_h, low, pltpu.roll(high, half, 1)).astype(BF16)
            o_mine[4 * j + 2 * q + 1, at, :] = jnp.where(left_h, pltpu.roll(low, half, 1), high).astype(BF16)

    def send_out(t, c):
        other = t * m + c
        return pltpu.make_async_remote_copy(
            src_ref=o_mine.at[t], dst_ref=o_all.at[me], send_sem=o_send.at[other],
            recv_sem=o_recv.at[me], device_id={"shell": t, "batch": c}, device_id_type=MESH,
        )

    pairs_of = n // 2
    for j in range(pairs_of):
        base = lax.rem(s // 2 + 1 + j, pairs_of) * 2
        done = back(base * 128, lambda q, r: inv[base + q, pl.ds(r, 1), :])
        for q in range(2):
            o_mine[base + q, 0:kc, :] = done[q].astype(BF16)
        if j < pairs_of - 1:
            for q in range(2):
                for c in range(m):
                    copy = send_out(base + q, c)
                    copy.start()
                    sends.append(copy)
    near = s // 2 * 2 + 1 - lax.rem(s, 2)
    for c in range(m):
        copy = send_out(near, c)
        copy.start()
        sends.append(copy)
    copy = send_out(s, 1 - b)
    copy.start()
    sends.append(copy)
    o_all[me] = o_mine[s]
    for o in range(1, nd):
        other = lax.rem(me + nd - o, nd)
        pltpu.make_async_remote_copy(
            src_ref=o_mine.at[0], dst_ref=o_all.at[other], send_sem=o_send.at[other],
            recv_sem=o_recv.at[other], device_id=partner, device_id_type=MESH,
        ).wait_recv()
    for d in range(nd):
        sums_ref[d * kc : d * kc + kc, :] = o_all[d, 0:kc, :]
        packed = o_all[d, kc : kc + kc // 2, :].astype(F32)
        w_out[d * kc : d * kc + kc // 2, :] = packed
        w_out[d * kc + kc // 2 : d * kc + kc, :] = pltpu.roll(packed, half, 1)
    for d in range(nd * kc // 128):
        wts_ref[:, d * 128 : d * 128 + 128] = w_out[d * 128 : d * 128 + 128, :].T[:half].astype(BF16)
    for copy in copies + relays + sends:
        copy.wait_send()


def fast_body(n, m, particles, classes, ctf, sigma2, shell_of, rot_table, ctf_group):
    width = shell_of.shape[0]
    rot = rot_table.shape[0]
    rows = particles.shape[0]
    k = classes.shape[0]
    groups = ctf.shape[0]
    kc = k // (n * m)
    total_rows = m * rows
    big = kc * rot
    nd = n * m
    wide = n * 128
    vmem = pl.BlockSpec(memory_space=pltpu.VMEM)
    dma = pltpu.SemaphoreType.DMA
    sums, wts, logev = pl.pallas_call(
        functools.partial(kernel, n, m, kc, rot),
        out_shape=(
            jax.ShapeDtypeStruct((k, 128), BF16),
            jax.ShapeDtypeStruct((width, k), BF16),
            jax.ShapeDtypeStruct((1, rows), F32),
        ),
        in_specs=[pl.BlockSpec(memory_space=pltpu.HBM)] * 7,
        out_specs=(vmem,) * 3,
        scratch_shapes=[
            pltpu.VMEM((rows, 128), BF16),
            pltpu.VMEM((k, 128), BF16),
            pltpu.VMEM((groups, width), F32),
            pltpu.VMEM((1, sigma2.shape[0]), F32),
            pltpu.VMEM((1, width), jnp.int32),
            pltpu.VMEM((rot, width), jnp.int32),
            pltpu.VMEM((1, rows), jnp.int32),
            dma((7,)),
            pltpu.VMEM((rot, 128), BF16),
            pltpu.VMEM((groups, 128), F32),
            pltpu.VMEM((1, 128), jnp.int32),
            pltpu.VMEM((m, 1, 128), jnp.int32),
            pltpu.VMEM((128, 128), F32),
            pltpu.VMEM((k, 128), F32),
            pltpu.VMEM((m, n, rows, 128), BF16),
            pltpu.VMEM((n, rot, 128), BF16),
            pltpu.VMEM((n, kc, 128), BF16),
            pltpu.VMEM((n, groups, 128), F32),
            pltpu.VMEM((m, rows, 128), BF16),
            pltpu.VMEM((n, rot, 128), jnp.int32),
            pltpu.VMEM((n, rot, 128), jnp.int32),
            pltpu.VMEM((n, kc, 128), F32),
            pltpu.VMEM((total_rows, wide), BF16),
            pltpu.VMEM((total_rows, wide + wide // 2), BF16),
            pltpu.VMEM((4 * groups, wide), BF16),
            pltpu.VMEM((big, wide), BF16),
            pltpu.VMEM((big, wide), BF16),
            pltpu.VMEM((big, wide), BF16),
            pltpu.VMEM((big, total_rows), F32),
            pltpu.VMEM((big, total_rows), BF16),
            pltpu.VMEM((big, 256), F32),
            pltpu.VMEM((8, total_rows), F32),
            pltpu.VMEM((nd, 8, total_rows), F32),
            pltpu.VMEM((n, kc + kc // 2, 128), BF16),
            pltpu.VMEM((nd, kc + kc // 2, 128), BF16),
            dma((4, n)),
            dma((4, n)),
            dma((n,)),
            dma((n,)),
            dma((2,)),
            dma((nd,)),
            dma((nd,)),
            dma((nd,)),
            dma((nd,)),
        ],
        compiler_params=pltpu.CompilerParams(
            collective_id=0, has_side_effects=True, vmem_limit_bytes=60 * 1024 * 1024
        ),
    )(particles, classes, ctf, sigma2[None, :], shell_of[None, :], rot_table, ctf_group[None, :])
    return sums.astype(F32), wts.T.astype(F32), logev[0]


def solution(mesh):
    in_specs = (
        P(("groups", "batch"), "shell"),
        P("groups", "shell"),
        P("groups", "shell"),
        P("groups"),
        P("shell"),
        P(None, "shell"),
        P(("groups", "batch")),
    )
    out_specs = (P("groups", "shell"), P("groups", "shell"), P(("groups", "batch")))
    n = mesh.shape["shell"]
    m = mesh.shape["batch"]

    def body(particles, classes, ctf, sigma2, shell_of, rot_table, ctf_group):
        args = (particles, classes, ctf, sigma2, shell_of, rot_table, ctf_group)
        per = classes.shape[0] // (n * m)
        fits = (
            m == 2
            and n % 4 == 0
            and n <= 16
            and classes.shape[0] % (n * m) == 0
            and per % 16 == 0
            and shell_of.shape[0] == 64
            and ctf.shape[0] == 8
            and particles.shape[0] % 16 == 0
            and particles.shape[0] <= 128
            and rot_table.shape[0] <= 128
            and classes.shape[0] % 128 == 0
            and sigma2.shape[0] % 8 == 0
            and rot_table.shape[0] % 48 == 0
            and per * rot_table.shape[0] % 384 == 0
        )
        if fits:
            return fast_body(n, m, *args)
        return plain_body(*args)

    return jax.shard_map(body, mesh=mesh, in_specs=in_specs, out_specs=out_specs, check_vma=False)
```

```python
import functools

import jax
import jax.numpy as jnp
from jax import lax
from jax.experimental import pallas as pl
from jax.experimental.pallas import tpu as pltpu
from jax.sharding import PartitionSpec as P

MESH = pl.DeviceIdType.MESH
BF16 = jnp.bfloat16
F32 = jnp.float32


def plain_body(particles, classes, ctf, sigma2, shell_of, rot_table, ctf_group):
    highest = lax.Precision.HIGHEST
    coef_width = shell_of.shape[0]
    class_count = classes.shape[0]
    rotations = rot_table.shape[0]
    levels = sigma2.shape[0]
    group_count = ctf.shape[0]
    offset = lax.axis_index("shell") * coef_width
    local_table = rot_table - offset
    pick_shell = (shell_of[:, None] == jnp.arange(levels, dtype=jnp.int32)[None, :]).astype(F32)
    weight = 1.0 / jnp.dot(pick_shell, sigma2, precision=highest, preferred_element_type=F32)
    pick_group = (ctf_group[:, None] == jnp.arange(group_count, dtype=jnp.int32)[None, :]).astype(F32)
    ctf_part = jnp.dot(pick_group, ctf, precision=highest, preferred_element_type=F32)
    values = particles.astype(F32)
    real_part = values[:, :coef_width]
    imag_part = values[:, coef_width:]
    weighted_ctf = weight[None, :] * ctf_part
    weighted = jnp.concatenate([weighted_ctf * real_part, weighted_ctf * imag_part], axis=1).astype(BF16)
    ctf_power = weight[None, :] * ctf * ctf
    sources = jnp.concatenate(
        [ctf_part * real_part, ctf_part * imag_part, ctf_part * ctf_part], axis=1
    ).astype(BF16)
    class_view = classes.reshape(class_count, 2, coef_width)
    rotated = jnp.take(class_view, local_table, axis=2)
    rotated = jnp.transpose(rotated, (0, 2, 1, 3)).reshape(class_count * rotations, 2 * coef_width)
    cross_terms = lax.dot_general(
        weighted, rotated, (((1,), (1,)), ((), ())), preferred_element_type=F32
    )
    rot_float = rotated.astype(F32)
    class_power = rot_float[:, :coef_width] ** 2 + rot_float[:, coef_width:] ** 2
    penalty = lax.dot_general(
        ctf_power, class_power, (((1,), (1,)), ((), ())), precision=highest, preferred_element_type=F32
    )
    total = lax.psum(
        cross_terms - 0.5 * jnp.dot(pick_group, penalty, precision=highest, preferred_element_type=F32),
        "shell",
    )
    peak = jnp.max(total, axis=1)
    log_evidence = peak + jnp.log(jnp.sum(jnp.exp(total - peak[:, None]), axis=1))
    posterior = jnp.exp(total - log_evidence[:, None]).astype(BF16)
    frames = lax.dot_general(
        posterior, sources, (((0,), (0,)), ((), ())), preferred_element_type=F32
    )
    frames = frames.reshape(class_count, rotations, 3, coef_width)
    placing = (
        local_table[:, :, None] == jnp.arange(coef_width, dtype=jnp.int32)[None, None, :]
    ).astype(F32)
    unrotated = jnp.einsum(
        "krqc,rcd->kqd", frames, placing, precision=highest, preferred_element_type=F32
    )
    sums_part = unrotated[:, 0:2].reshape(class_count, 2 * coef_width)
    weights_part = unrotated[:, 2]
    class_sums, class_weights = lax.psum((sums_part, weights_part), "batch")
    return (class_sums, class_weights, log_evidence)


def split3(x):
    one = x.astype(BF16).astype(F32)
    two = (x - one).astype(BF16).astype(F32)
    return one, two, x - one - two


def gather_lanes(x, index):
    return jnp.take_along_axis(x, index, axis=1, mode="promise_in_bounds")


def kernel(
    n, m, kc, rot, part_in, cls_in, ctf_in, sigma_in, shell_in, table_in, group_in,
    sums_ref, wts_ref, logev_ref,
    part_ref, cls_ref, ctf_ref, sigma_ref, shell_ref, table_ref, group_ref, load_sem,
    tab_ref, cw_ref, grp_ref, g_grp, square, w_out, g_part, g_tab, g_cls, g_cw, g_pick, fwd, inv, cls32, w_s, s_s, p_s, r_s, hi_s, lo_s, sc_s, post_s, frame,
    st_mine, st_all, o_mine, o_all,
    in_send, in_recv, relay_send, relay_recv, pick_sem, st_send, st_recv, o_send, o_recv,
):
    s = lax.axis_index("shell")
    b = lax.axis_index("batch")
    rows = part_ref.shape[0]
    total_rows = m * rows
    half = 64
    me = s * m + b
    nd = n * m
    lane = lambda shape: lax.broadcasted_iota(jnp.int32, shape, len(shape) - 1)

    def peer(o):
        other = lax.rem(me + o, nd)
        return other, {"shell": other // m, "batch": lax.rem(other, m)}

    loads = [
        pltpu.make_async_copy(src, dst, load_sem.at[j])
        for j, (src, dst) in enumerate(
            (
                (table_in, table_ref), (sigma_in, sigma_ref), (shell_in, shell_ref), (ctf_in, ctf_ref),
                (group_in, group_ref), (cls_in, cls_ref), (part_in, part_ref),
            )
        )
    ]
    for load in loads:
        load.start()
    barrier = pltpu.get_barrier_semaphore()
    for o in range(1, nd):
        pl.semaphore_signal(barrier, inc=1, device_id=peer(o)[1], device_id_type=MESH)

    def sub(shape):
        return lax.broadcasted_iota(jnp.int32, shape, 0)

    for load in loads:
        load.wait()
    table = (table_ref[...] - s * half).astype(F32)
    table = jnp.concatenate([table, jnp.zeros_like(table)], axis=1)
    tall = jnp.concatenate([table, jnp.zeros((128 - rot, 128), F32)], axis=0)
    square[...] = tall.T
    spots = sub((half, 128)).astype(F32)
    found = jnp.zeros((half, 128), F32)
    for c in range(half):
        found = jnp.where(square[c : c + 1, :] == spots, float(c), found)
    back_table = jnp.concatenate([found, jnp.zeros_like(found)], axis=0).T[:rot]
    tab_ref[...] = (table + pltpu.roll(back_table, half, 1)).astype(BF16)
    levels = sigma_ref.shape[1]
    chosen_level = (shell_ref[...] == sub((levels, half))).astype(F32).astype(BF16)
    one, two, three = split3(sigma_ref[...])
    order = sub((8, levels))
    stack = jnp.where(order == 0, one, jnp.where(order == 1, two, jnp.where(order == 2, three, 0.0)))
    chosen = jnp.dot(stack.astype(BF16), chosen_level, preferred_element_type=F32)
    weight = 1.0 / jnp.sum(chosen, axis=0, keepdims=True)
    ctf = ctf_ref[...]
    cw_ref[...] = jnp.concatenate([ctf, jnp.broadcast_to(weight, ctf.shape)], axis=1)
    grp_ref[...] = jnp.zeros_like(grp_ref)
    grp_ref[:, :rows] = group_ref[...]

    pl.semaphore_wait(barrier, nd - 1)

    copies = []

    def send_in(j, o):
        t = lax.rem(s + o, n)
        first = pl.multiple_of((t * m + b) * kc, kc)
        pairs = (
            (cls_ref.at[pl.ds(first, kc)], g_cls.at[s]),
            (cw_ref, g_cw.at[s]),
            (tab_ref, g_tab.at[s]),
            (part_ref, g_part.at[b, s]),
        )
        copy = pltpu.make_async_remote_copy(
            src_ref=pairs[j][0], dst_ref=pairs[j][1], send_sem=in_send.at[j, t], recv_sem=in_recv.at[j, s],
            device_id={"shell": t, "batch": b}, device_id_type=MESH,
        )
        copy.start()
        copies.append(copy)

    for o in range(1, n):
        for j in range(3):
            send_in(j, o)
    for o in range(1, n):
        send_in(3, o)
    partner = {"shell": s, "batch": 1 - b}
    pick_copy = pltpu.make_async_remote_copy(
        src_ref=grp_ref, dst_ref=g_grp.at[b], send_sem=pick_sem.at[0], recv_sem=pick_sem.at[1],
        device_id=partner, device_id_type=MESH,
    )
    pick_copy.start()
    relays = []

    def relay(src, t):
        copy = pltpu.make_async_remote_copy(
            src_ref=src, dst_ref=g_part.at[b, t], send_sem=relay_send.at[t], recv_sem=relay_recv.at[t],
            device_id=partner, device_id_type=MESH,
        )
        copy.start()
        relays.append(copy)

    relay(part_ref, s)
    g_part[b, s] = part_ref[...]
    g_grp[b] = grp_ref[...]
    g_tab[s] = tab_ref[...]
    g_cw[s] = cw_ref[...]
    g_cls[s] = cls_ref[pl.ds(pl.multiple_of(me * kc, kc), kc), :]

    def arrive(j, t):
        refs = (g_cls.at[t], g_cw.at[t], g_tab.at[t], g_part.at[b, t])
        pltpu.make_async_remote_copy(
            src_ref=refs[j], dst_ref=refs[j], send_sem=in_send.at[j, t], recv_sem=in_recv.at[j, t],
            device_id=partner, device_id_type=MESH,
        ).wait_recv()

    for o in range(1, n):
        t = lax.rem(s + n - o, n)
        arrive(0, t)
        arrive(1, t)
        arrive(2, t)

    left = lane((rot, 128)) < half
    for t in range(n):
        tab = g_tab[t].astype(F32)
        swap = pltpu.roll(tab, half, 1)
        fwd[t] = jnp.where(left, tab, swap + half).astype(jnp.int32)
        inv[t] = jnp.where(left, swap, tab + half).astype(jnp.int32)
        cls32[t] = g_cls[t].astype(F32)

    def rotate(i, carry):
        for u in range(4):
            r = i * 4 + u
            at = pl.ds(pl.multiple_of(r * kc, kc), kc)
            for t in range(n):
                index = jnp.broadcast_to(fwd[t, pl.ds(r, 1), :], (kc, 128))
                turned = gather_lanes(cls32[t], index)
                power = turned * turned
                high = power.astype(BF16)
                cols = slice(t * 128, t * 128 + 128)
                r_s[at, cols] = turned.astype(BF16)
                hi_s[at, cols] = high
                lo_s[at, cols] = (power - high.astype(F32)).astype(BF16)
        return carry

    lax.fori_loop(0, rot // 4, rotate, 0)

    for o in range(1, n):
        t = lax.rem(s + n - o, n)
        arrive(3, t)
        relay(g_part.at[b, t], t)
    pick_copy.wait()
    place = sub((128, 128))
    for c in range(m):
        member = (g_grp[c] == (place & 7)) & (place < 24)
        g_pick[c] = member.astype(F32).T[:rows].astype(BF16)
    for o in range(n):
        t = lax.rem(s + o, n)
        pltpu.make_async_remote_copy(
            src_ref=g_part.at[1 - b, t], dst_ref=g_part.at[1 - b, t],
            send_sem=relay_send.at[t], recv_sem=relay_recv.at[t],
            device_id=partner, device_id_type=MESH,
        ).wait_recv()

    pick = g_pick[...].reshape(total_rows, 128)[:, :32]
    left8 = lane((8, 128)) < half
    left_p = lane((total_rows, 128)) < half
    before = None
    for t in range(n):
        packed = g_cw[t]
        swap = pltpu.roll(packed, half, 1)
        ctf = jnp.where(left8, packed, swap)
        weight = jnp.where(left8, swap, packed)
        zero = jnp.zeros_like(ctf)
        pieces = jnp.concatenate(split3(ctf) + (zero,), axis=0).astype(BF16)
        ctf_part = jnp.dot(pick, pieces, preferred_element_type=F32)
        values = g_part[:, t].reshape(total_rows, 128).astype(F32)
        cols = slice(t * 128, t * 128 + 128)
        w_s[:, cols] = (weight[0:1] * ctf_part * values).astype(BF16)
        s_s[:, cols] = (ctf_part * values).astype(BF16)
        p_s[:, cols] = jnp.concatenate(split3(weight * ctf * ctf) + (zero,), axis=0).astype(BF16)
        if t % 2 == 1:
            mixed = jnp.where(left_p, before, ctf_part)
            cols = slice(n * 128 + t // 2 * 128, n * 128 + t // 2 * 128 + 128)
            s_s[:, cols] = (mixed * mixed).astype(BF16)
        before = ctf_part

    nt = (((1,), (1,)), ((), ()))
    chunk = 384
    big = kc * rot

    def score(i, peak):
        at = pl.ds(i * chunk, chunk)
        cross = lax.dot_general(r_s[at, :], w_s[...], nt, preferred_element_type=F32)
        pen = lax.dot_general(hi_s[at, :], p_s[...], nt, preferred_element_type=F32)
        pen = pen + lax.dot_general(lo_s[at, :], p_s[...], nt, preferred_element_type=F32)
        spread = 0.0
        for piece in split3(pen):
            spread = spread + lax.dot_general(piece.astype(BF16), pick, nt, preferred_element_type=F32)
        total = cross - 0.5 * spread
        sc_s[at, :] = total
        return jnp.maximum(peak, jnp.max(total, axis=0, keepdims=True))

    peak = jnp.full((1, total_rows), -jnp.inf, F32)
    for i in range(big // chunk):
        peak = score(i, peak)
    summed = jnp.sum(jnp.exp(sc_s[...] - peak), axis=0, keepdims=True)
    st_mine[0:1, :] = peak
    st_mine[1:2, :] = summed
    st_mine[2:8, :] = jnp.zeros((6, total_rows), F32)

    sends = []
    for o in range(1, nd):
        other, dest = peer(o)
        copy = pltpu.make_async_remote_copy(
            src_ref=st_mine, dst_ref=st_all.at[me], send_sem=st_send.at[other], recv_sem=st_recv.at[me],
            device_id=dest, device_id_type=MESH,
        )
        copy.start()
        sends.append(copy)
    st_all[me] = st_mine[...]
    for o in range(1, nd):
        other = lax.rem(me + nd - o, nd)
        pltpu.make_async_remote_copy(
            src_ref=st_mine, dst_ref=st_all.at[other], send_sem=st_send.at[other], recv_sem=st_recv.at[other],
            device_id=partner, device_id_type=MESH,
        ).wait_recv()
    peaks = st_all[:, 0, :]
    top = jnp.max(peaks, axis=0, keepdims=True)
    whole = jnp.sum(st_all[:, 1, :] * jnp.exp(peaks - top), axis=0, keepdims=True)
    logev = top + jnp.log(whole)
    logev_ref[...] = jnp.where(b == 0, logev[:, :rows], logev[:, rows:])
    post_s[...] = jnp.exp(sc_s[...] - logev).astype(BF16)

    def back(first, index_of):
        cols = pl.ds(pl.multiple_of(first, 256), 256)
        frame[...] = jnp.dot(post_s[...], s_s[:, cols], preferred_element_type=F32)

        def step(i, carry):
            out = list(carry)
            for r in range(rot):
                at = pl.ds(r * kc, kc)
                for q in range(2):
                    index = jnp.broadcast_to(index_of(q, r), (kc, 128))
                    out[q] = out[q] + gather_lanes(frame[at, q * 128 : q * 128 + 128], index)
            return tuple(out)

        zero = jnp.zeros((kc, 128), F32)
        return step(0, (zero, zero))

    left1 = lane((1, 128)) < half
    left_h = lane((kc // 2, 128)) < half
    for j in range(n // 4):
        done = back(
            n * 128 + j * 256,
            lambda q, r: jnp.where(
                left1, inv[4 * j + 2 * q, pl.ds(r, 1), :], inv[4 * j + 2 * q + 1, pl.ds(r, 1), :]
            ),
        )
        for q in range(2):
            low, high = done[q][: kc // 2], done[q][kc // 2 :]
            at = slice(kc, kc + kc // 2)
            o_mine[4 * j + 2 * q, at, :] = jnp.where(left_h, low, pltpu.roll(high, half, 1)).astype(BF16)
            o_mine[4 * j + 2 * q + 1, at, :] = jnp.where(left_h, pltpu.roll(low, half, 1), high).astype(BF16)

    def send_out(t, c):
        other = t * m + c
        return pltpu.make_async_remote_copy(
            src_ref=o_mine.at[t], dst_ref=o_all.at[me], send_sem=o_send.at[other],
            recv_sem=o_recv.at[me], device_id={"shell": t, "batch": c}, device_id_type=MESH,
        )

    pairs_of = n // 2
    for j in range(pairs_of):
        base = lax.rem(s // 2 + 1 + j, pairs_of) * 2
        done = back(base * 128, lambda q, r: inv[base + q, pl.ds(r, 1), :])
        for q in range(2):
            o_mine[base + q, 0:kc, :] = done[q].astype(BF16)
        if j < pairs_of - 1:
            for q in range(2):
                for c in range(m):
                    copy = send_out(base + q, c)
                    copy.start()
                    sends.append(copy)
    near = s // 2 * 2 + 1 - lax.rem(s, 2)
    for c in range(m):
        copy = send_out(near, c)
        copy.start()
        sends.append(copy)
    copy = send_out(s, 1 - b)
    copy.start()
    sends.append(copy)
    o_all[me] = o_mine[s]
    for o in range(1, nd):
        other = lax.rem(me + nd - o, nd)
        pltpu.make_async_remote_copy(
            src_ref=o_mine.at[0], dst_ref=o_all.at[other], send_sem=o_send.at[other],
            recv_sem=o_recv.at[other], device_id=partner, device_id_type=MESH,
        ).wait_recv()
    for d in range(nd):
        sums_ref[d * kc : d * kc + kc, :] = o_all[d, 0:kc, :]
        packed = o_all[d, kc : kc + kc // 2, :].astype(F32)
        w_out[d * kc : d * kc + kc // 2, :] = packed
        w_out[d * kc + kc // 2 : d * kc + kc, :] = pltpu.roll(packed, half, 1)
    for d in range(nd * kc // 128):
        wts_ref[:, d * 128 : d * 128 + 128] = w_out[d * 128 : d * 128 + 128, :].T[:half].astype(BF16)
    for copy in copies + relays + sends:
        copy.wait_send()


def fast_body(n, m, particles, classes, ctf, sigma2, shell_of, rot_table, ctf_group):
    width = shell_of.shape[0]
    rot = rot_table.shape[0]
    rows = particles.shape[0]
    k = classes.shape[0]
    groups = ctf.shape[0]
    kc = k // (n * m)
    total_rows = m * rows
    big = kc * rot
    nd = n * m
    wide = n * 128
    vmem = pl.BlockSpec(memory_space=pltpu.VMEM)
    dma = pltpu.SemaphoreType.DMA
    sums, wts, logev = pl.pallas_call(
        functools.partial(kernel, n, m, kc, rot),
        out_shape=(
            jax.ShapeDtypeStruct((k, 128), BF16),
            jax.ShapeDtypeStruct((width, k), BF16),
            jax.ShapeDtypeStruct((1, rows), F32),
        ),
        in_specs=[pl.BlockSpec(memory_space=pltpu.HBM)] * 7,
        out_specs=(vmem,) * 3,
        scratch_shapes=[
            pltpu.VMEM((rows, 128), BF16),
            pltpu.VMEM((k, 128), BF16),
            pltpu.VMEM((groups, width), F32),
            pltpu.VMEM((1, sigma2.shape[0]), F32),
            pltpu.VMEM((1, width), jnp.int32),
            pltpu.VMEM((rot, width), jnp.int32),
            pltpu.VMEM((1, rows), jnp.int32),
            dma((7,)),
            pltpu.VMEM((rot, 128), BF16),
            pltpu.VMEM((groups, 128), F32),
            pltpu.VMEM((1, 128), jnp.int32),
            pltpu.VMEM((m, 1, 128), jnp.int32),
            pltpu.VMEM((128, 128), F32),
            pltpu.VMEM((k, 128), F32),
            pltpu.VMEM((m, n, rows, 128), BF16),
            pltpu.VMEM((n, rot, 128), BF16),
            pltpu.VMEM((n, kc, 128), BF16),
            pltpu.VMEM((n, groups, 128), F32),
            pltpu.VMEM((m, rows, 128), BF16),
            pltpu.VMEM((n, rot, 128), jnp.int32),
            pltpu.VMEM((n, rot, 128), jnp.int32),
            pltpu.VMEM((n, kc, 128), F32),
            pltpu.VMEM((total_rows, wide), BF16),
            pltpu.VMEM((total_rows, wide + wide // 2), BF16),
            pltpu.VMEM((4 * groups, wide), BF16),
            pltpu.VMEM((big, wide), BF16),
            pltpu.VMEM((big, wide), BF16),
            pltpu.VMEM((big, wide), BF16),
            pltpu.VMEM((big, total_rows), F32),
            pltpu.VMEM((big, total_rows), BF16),
            pltpu.VMEM((big, 256), F32),
            pltpu.VMEM((8, total_rows), F32),
            pltpu.VMEM((nd, 8, total_rows), F32),
            pltpu.VMEM((n, kc + kc // 2, 128), BF16),
            pltpu.VMEM((nd, kc + kc // 2, 128), BF16),
            dma((4, n)),
            dma((4, n)),
            dma((n,)),
            dma((n,)),
            dma((2,)),
            dma((nd,)),
            dma((nd,)),
            dma((nd,)),
            dma((nd,)),
        ],
        compiler_params=pltpu.CompilerParams(
            collective_id=0, has_side_effects=True, vmem_limit_bytes=60 * 1024 * 1024
        ),
    )(particles, classes, ctf, sigma2[None, :], shell_of[None, :], rot_table, ctf_group[None, :])
    return sums.astype(F32), wts.T.astype(F32), logev[0]


def solution(mesh):
    in_specs = (
        P(("groups", "batch"), "shell"),
        P("groups", "shell"),
        P("groups", "shell"),
        P("groups"),
        P("shell"),
        P(None, "shell"),
        P(("groups", "batch")),
    )
    out_specs = (P("groups", "shell"), P("groups", "shell"), P(("groups", "batch")))
    n = mesh.shape["shell"]
    m = mesh.shape["batch"]

    def body(particles, classes, ctf, sigma2, shell_of, rot_table, ctf_group):
        args = (particles, classes, ctf, sigma2, shell_of, rot_table, ctf_group)
        per = classes.shape[0] // (n * m)
        fits = (
            m == 2
            and n % 4 == 0
            and n <= 16
            and classes.shape[0] % (n * m) == 0
            and per % 16 == 0
            and shell_of.shape[0] == 64
            and ctf.shape[0] == 8
            and particles.shape[0] % 16 == 0
            and particles.shape[0] <= 128
            and rot_table.shape[0] <= 128
            and classes.shape[0] % 128 == 0
            and sigma2.shape[0] % 8 == 0
            and rot_table.shape[0] % 48 == 0
            and per * rot_table.shape[0] % 384 == 0
        )
        if fits:
            return fast_body(n, m, *args)
        return plain_body(*args)

    return jax.shard_map(body, mesh=mesh, in_specs=in_specs, out_specs=out_specs, check_vma=False)
```
